256 devices in a mesh: grp: 2 (over y), seq: 128 (over z, x, core).
Axes of the slice: x: 4, y: 2, z: 16, core: 2. Of those that a mesh axis runs over, the one named last changes fastest.
The devices are a block of a 4x16x16 slice.
Arguments:
- frames: bfloat16 [4, 81920, 1280], P('grp', 'seq'), parts along dimension 0, may hold values from -120 to 120
- dec_states: bfloat16 [2, 256, 1280], P(None, 'grp'), parts along dimension 1, may hold values from -6 to 6
- w_query: bfloat16 [1280, 1280], P(None, 'seq'), may hold values from -0.15625 to 0.15625
- w_keyval: bfloat16 [1280, 2560], replicated, may hold values from -0.15625 to 0.15625
- w_output: bfloat16 [1280, 1280], P(None, 'seq'), may hold values from -0.15625 to 0.15625
- head_slope: float32 [20], replicated, may hold values from 0.3 to 12
- lengths: int32 [4, 128], P('grp'), parts along dimension 0, may hold values from 128 to 640, as said below
- positions: int32 [2, 256], P(None, 'grp'), parts along dimension 1, may hold values from 0 to 127
Outputs:
- attended: bfloat16 [2, 256, 1280], P(None, 'grp', 'seq'), parts along dimension 1
The draws below stay inside these ranges and needn't reach their ends.
There are 2 independent parts, one for each index of `grp`. The reference program is written for one: setup_inputs(seed, part) draws one part's arguments, and reference() takes and returns one part's arrays. A program takes and returns all parts, laid end to end along the dimension named above; an argument that names none is the same for every part. Nothing has to cross between parts.
Inputs may be any that keep to these rules, and one draw needn't show every extreme that they name: `lengths`: every step has one block of exactly 640 valid frames.
All inputs are finite; a program needn't handle non-finite values.
Results may differ from the reference program's by a relative error of at most 0.005.
The reference program's roundings to bfloat16 on the way count: a program that leaves them out, or rounds other values in their place, can miss the bound.
Values may be sent and summed in bfloat16 or wider, within the bound.
A program may use at most 128 MiB of HBM per device.

```python
import math
import jax
import jax.numpy as jnp
from jax import lax

D = 1280
H = 20
FR = 640
STEPS = 2
QROWS = 128
N_SEQ = 128


def draw_frames(key, part):
    key_base = jax.random.fold_in(key, 11)
    base = jax.random.normal(key_base, (STEPS, N_SEQ * FR, D), jnp.float32)
    base = jnp.clip(base, -6.0, 6.0)
    return base.astype(jnp.bfloat16)


def draw_lengths(key, part):
    key_pick = jax.random.fold_in(key, 21)
    key_long = jax.random.fold_in(key, 22)
    lowest = FR // 5
    spread = FR - lowest
    picked = jax.random.randint(key_pick, (STEPS, N_SEQ), 0, spread + 1)
    frame_counts = lowest + picked * picked // spread
    longest = jax.random.randint(key_long, (STEPS,), 0, N_SEQ)
    longest_at = jnp.arange(N_SEQ, dtype=jnp.int32)[None, :] == longest[:, None]
    return jnp.where(longest_at, FR, frame_counts).astype(jnp.int32)


def plant(values, own_key, smallest, high):
    spot = [jax.random.randint(jax.random.fold_in(own_key, axis), (), 0, length) for axis, length in enumerate(values.shape)]
    main_axis = values.shape.index(max(values.shape))
    neighbour = spot[:main_axis] + [(spot[main_axis] + 1) % values.shape[main_axis]] + spot[main_axis + 1:]
    return values.at[tuple(spot)].set(smallest).at[tuple(neighbour)].set(high)


def block_levels(own_key, extent, split, least, largest):
    level, own = 1.0, jax.random.fold_in(own_key, 6)
    for axis_at, shards_of in split:
        draws = jnp.exp(jax.random.uniform(jax.random.fold_in(own, axis_at), (shards_of,), jnp.float32, least / len(split), largest / len(split)))
        level = level * jnp.repeat(draws, extent[axis_at] // shards_of).reshape([-1 if axis == axis_at else 1 for axis in range(len(extent))])
    return level


def noise(rng, shape, scale, most, pieces=(), kind=jnp.bfloat16):
    result = jax.random.normal(rng, shape, jnp.float32) * scale
    if len(pieces) > 0:
        result = block_levels(rng, shape, pieces, -0.22, 0.18) * result
    return jnp.clip(result, min=-most, max=most).astype(kind)


def setup_inputs(seed: int = 0, part: int = 0) -> dict:
    splits = jax.random.split(jax.random.key(seed), 9)
    part_splits = jax.random.split(jax.random.fold_in(splits[8], part), 9)
    return {
        "frames": draw_frames(jax.random.fold_in(jax.random.fold_in(splits[8], part), 71), part),
        "dec_states": noise(part_splits[1], (STEPS, QROWS, D), 1.0, 6.0),
        "w_query": noise(splits[2], (D, D), D ** -0.5, 0.15625, ((1, 128),)),
        "w_keyval": noise(splits[3], (D, 2 * D), D ** -0.5, 0.15625),
        "w_output": noise(splits[4], (D, D), D ** -0.5, 0.15625, ((1, 128),)),
        "head_slope": jnp.clip(jnp.exp(jax.random.uniform(splits[5], (H,), jnp.float32, math.log(0.3), math.log(12.0))), 0.3, 12.0),
        "lengths": draw_lengths(jax.random.fold_in(jax.random.fold_in(splits[8], part), 71), part),
        "positions": plant(jax.random.randint(part_splits[7], (STEPS, QROWS), 0, N_SEQ), jax.random.fold_in(part_splits[7], 1), 0, N_SEQ - 1).astype(jnp.int32),
    }


def reference(frames, dec_states, w_query, w_keyval, w_output, head_slope, lengths, positions):
    step_count, total_frames, model_width = frames.shape
    query_rows = dec_states.shape[1]
    head_count = head_slope.shape[0]
    head_size = model_width // head_count
    block_count = N_SEQ
    frame_count = total_frames // block_count
    keyval = jnp.dot(frames.reshape(step_count * total_frames, model_width), w_keyval, preferred_element_type=jnp.float32).astype(jnp.bfloat16)
    all_keys = keyval[:, :model_width].reshape(step_count, block_count, frame_count, head_count, head_size)
    all_values = keyval[:, model_width:].reshape(step_count, block_count, frame_count, head_count, head_size)
    queries = jnp.dot(dec_states.reshape(step_count * query_rows, model_width), w_query, preferred_element_type=jnp.float32).astype(jnp.bfloat16)
    queries = queries.reshape(step_count, query_rows, head_count, head_size)
    results = []
    for step_now in range(step_count):
        query_now = queries[step_now].astype(jnp.float32)
        row_positions = positions[step_now].astype(jnp.float32)

        def one_block(flat_index):
            older_step = flat_index // block_count
            block_index = flat_index % block_count
            block_keys = all_keys[older_step, block_index].astype(jnp.float32)
            block_values = all_values[older_step, block_index].astype(jnp.float32)
            scores = jnp.einsum('qhd,jhd->hqj', query_now, block_keys) / math.sqrt(head_size)
            slot_place = ((block_index + 1) % block_count).astype(jnp.float32)
            age_steps = (step_now - older_step).astype(jnp.float32)
            distance = jnp.abs(row_positions - slot_place) / block_count + age_steps
            scores = scores - head_slope[:, None, None] * distance[None, :, None]
            length_now = lengths[older_step, block_index]
            valid = jnp.arange(frame_count, dtype=jnp.int32)[None, None, :] < length_now
            scores = jnp.where(valid, scores, -jnp.inf)
            row_peak = lax.optimization_barrier(jnp.max(scores, axis=2))
            weights = jnp.exp(scores - row_peak[:, :, None]).astype(jnp.bfloat16).astype(jnp.float32)
            row_total = lax.optimization_barrier(jnp.sum(weights, axis=2))
            row_context = jnp.einsum('hqj,jhd->hqd', weights, block_values)
            return (row_peak, row_total, row_context)
        peaks, totals, contexts = lax.map(one_block, jnp.arange((step_now + 1) * block_count, dtype=jnp.int32))
        row_top = lax.optimization_barrier(jnp.max(peaks, axis=0))
        factors = jnp.exp(peaks - row_top[None])
        row_total = lax.optimization_barrier(jnp.sum(factors * totals, axis=0))
        row_context = lax.optimization_barrier(jnp.sum(factors[..., None] * contexts, axis=0))
        context = (row_context / row_total[..., None]).transpose(1, 0, 2).reshape(query_rows, model_width)
        context = context.astype(jnp.bfloat16)
        results.append(jnp.dot(context, w_output, preferred_element_type=jnp.float32).astype(jnp.bfloat16))
    return jnp.stack(results)
```

```python
import functools

import jax
import jax.numpy as jnp
from jax import lax
from jax.experimental import pallas as pl
from jax.experimental.pallas import tpu as pltpu
from jax.sharding import Mesh
from jax.sharding import PartitionSpec as P

SEQ = ("z", "x", "c")
F32, BF16 = jnp.float32, jnp.bfloat16
HD = 64
CP = 16
NB = 16
COLS = 256
ROWS = 256
LOW = -1e30


def mm(a, b):
    return jnp.dot(a, b, preferred_element_type=F32)


def mm_t(a, b):
    return lax.dot_general(a, b, (((1,), (1,)), ((), ())), preferred_element_type=F32)


def iota(shape, dim):
    return lax.broadcasted_iota(jnp.int32, shape, dim)


def remote(src, dst, send, recv, device):
    return pltpu.make_async_remote_copy(
        src_ref=src,
        dst_ref=dst,
        send_sem=send,
        recv_sem=recv,
        device_id=device,
        device_id_type=pl.DeviceIdType.MESH,
    )


def near_first(n):
    order = []
    for d in range(1, n // 2 + 1):
        order.append(d)
        if n - d != d:
            order.append(n - d)
    return order


def pieces(value, count):
    parts = []
    for _ in range(count):
        part = value.astype(BF16).astype(F32)
        parts.append(part)
        value = value - part
    return parts


def stats_tile(peak, total, rows):
    at = iota((rows, peak.shape[-1]), 0)
    tile = jnp.zeros((rows, peak.shape[-1]), F32)
    for k, part in enumerate(pieces(peak, 3) + pieces(total, 2)):
        tile = jnp.where(at == k, part, tile)
    return tile


def kernel(
    sizes,
    frames, wkv, dec, wq, wo, pos, lens, slope,
    out,
    fr, wt, keys, vals, mask, grid_q, qpad, part, pair_in, xs, xr, zs, zr, ctx, wo_in, wo_all, o_out, o_in,
    fr_sem, wt_sem, qz_s, qz_r, qx_s, qx_r, qc_s, qc_r, wo_s, wo_r, pc_s, pc_r, x_s, x_r, z_s, z_r, g_s, g_r, h_s, h_r, o_s, o_r,
):
    nz, nx, nc, steps, frame_rows, tokens, width, heads, chunk = sizes
    n = nz * nx * nc
    z, x, c = lax.axis_index("z"), lax.axis_index("x"), lax.axis_index("c")
    own = (z * nx + x) * nc + c
    other = 1 - c
    near = near_first(nz)
    far = near[::-1]
    hpx = heads // nx
    pairs = heads // 2
    slots = hpx * HD
    span = zs.shape[-1]
    per_z = tokens // nz
    tall = steps * frame_rows

    loads = []
    for k in range(tall // ROWS):
        rows = pl.ds(k * ROWS, ROWS)
        loads.append(pltpu.make_async_copy(frames.at[rows, :], fr.at[rows, :], fr_sem.at[k]))
    tiles = 2 * width // COLS
    for load in loads:
        load.start()

    def tile_load(j):
        cols = pl.ds(pl.multiple_of(j * COLS, COLS), COLS)
        return pltpu.make_async_copy(wkv.at[:, cols], wt.at[:, cols], wt_sem.at[j])

    for j in range(tiles):
        tile_load(j).start()

    barrier = pltpu.get_barrier_semaphore()
    for d in far:
        pl.semaphore_signal(barrier, inc=1, device_id={"z": lax.rem(z + d, nz)}, device_id_type=pl.DeviceIdType.MESH)
    for d in range(1, nx):
        pl.semaphore_signal(barrier, inc=1, device_id={"x": lax.rem(x + d, nx)}, device_id_type=pl.DeviceIdType.MESH)
    pl.semaphore_signal(barrier, inc=1, device_id={"c": other}, device_id_type=pl.DeviceIdType.MESH)

    qpad[...] = jnp.zeros_like(qpad)
    qpad[:chunk] = mm_t(wq[...], dec[...])
    grid_q[own] = qpad[...].astype(BF16)
    grid_q[pl.ds(n, grid_q.shape[0] - n)] = jnp.zeros((grid_q.shape[0] - n, CP, grid_q.shape[2]), BF16)

    at_lane = iota((frame_rows, 128), 1)
    at_row = iota((frame_rows, 128), 0)
    for t in range(steps):
        hidden = (at_lane == 0) & (at_row >= lens[t, own])
        mask[t] = jnp.where(hidden, LOW, 0.0).astype(BF16)

    for load in loads:
        load.wait()

    def project_keys(j, carry):
        tile_load(j).wait()
        cols = pl.ds(pl.multiple_of(j * COLS, COLS), COLS)

        def rows_of(m, carry):
            rows = pl.ds(pl.multiple_of(m * ROWS, ROWS), ROWS)
            keys[rows, cols] = mm(fr[rows, :], wt[:, cols]).astype(BF16)
            return carry

        return lax.fori_loop(0, tall // ROWS, rows_of, carry)

    def project_values(j, carry):
        tile_load(j + tiles // 2).wait()
        cols = pl.ds(pl.multiple_of(j * COLS + width, COLS), COLS)
        head_rows = pl.ds(pl.multiple_of(j * COLS, COLS), COLS)

        def rows_of(m, carry):
            rows = pl.ds(pl.multiple_of(m * ROWS, ROWS), ROWS)
            vals[head_rows, rows] = mm(fr[rows, :], wt[:, cols]).T.astype(BF16)
            return carry

        return lax.fori_loop(0, tall // ROWS, rows_of, carry)

    lax.fori_loop(0, tiles // 2, project_keys, 0)

    pl.semaphore_wait(barrier, nz - 1 + nx - 1 + 1)

    def q_chunk(zz, xx, cc):
        return grid_q.at[(zz * nx + xx) * nc + cc]

    def q_over_z(k, zz):
        return remote(q_chunk(z, x, c), q_chunk(z, x, c), qz_s.at[k], qz_r.at[z], {"z": zz})

    for d in far:
        q_over_z(d, lax.rem(z + d, nz)).start()
    to_partner = remote(wo, wo_in, wo_s, wo_r, {"c": other})
    to_partner.start()

    lax.fori_loop(0, tiles // 2, project_values, 0)

    def q_over_x(zz, d):
        here = q_chunk(zz, x, c)
        return remote(here, here, qx_s.at[zz, d], qx_r.at[zz, x], {"x": lax.rem(x + d, nx)})

    def q_over_c(zz, xx):
        here = q_chunk(zz, xx, c)
        return remote(here, here, qc_s.at[zz, xx], qc_r.at[zz, xx], {"c": other})

    for d in [0] + near:
        zz = lax.rem(z + d, nz)
        if d:
            here = q_chunk(zz, x, c)
            remote(here, here, qz_s.at[d], qz_r.at[zz], {"z": zz}).wait_recv()
        for e in range(1, nx):
            q_over_x(zz, e).start()
        q_over_c(zz, x).start()
    for d in [0] + near:
        zz = lax.rem(z + d, nz)
        for e in range(1, nx):
            xx = lax.rem(x + e, nx)
            here = q_chunk(zz, xx, c)
            remote(here, here, qx_s.at[zz, e], qx_r.at[zz, xx], {"x": xx}).wait_recv()
            q_over_c(zz, xx).start()

    to_partner.wait_recv()
    wo_all[...] = jnp.zeros_like(wo_all)
    for xx in range(nx):
        for i in range(hpx):
            cols = pl.ds((i * nx + xx) * HD, HD)
            wo_all[xx, :chunk, pl.ds(i * HD, HD)] = wo[:, cols]
            wo_all[xx, CP : CP + chunk, pl.ds(i * HD, HD)] = wo_in[:, cols]

    for d in [0] + near:
        zz = lax.rem(z + d, nz)
        for xx in range(nx):
            here = q_chunk(zz, xx, other)
            remote(here, here, qc_s.at[zz, xx], qc_r.at[zz, xx], {"c": other}).wait_recv()

    place = lax.rem(own + 1, n).astype(F32)
    dist = [jnp.abs(pos[pl.ds(s, 1), :].astype(F32) - place) / n for s in range(steps)]
    ones_rows = jnp.ones((16, frame_rows), BF16)
    lane = iota((2 * HD, steps * tokens), 1)
    row = iota((2 * HD, steps * tokens), 0)
    sel_lane = iota((2 * HD, NB * CP), 1)
    sel_row = iota((2 * HD, NB * CP), 0)
    unit = jnp.where(row == 0, 1.0, 0.0).astype(BF16)

    def weigh(t, p, rhs):
        at = pl.ds(pl.multiple_of(p * 2 * HD, 2 * HD), 2 * HD)
        lhs = jnp.concatenate([keys[pl.ds(t * frame_rows, frame_rows), at], mask[t]], axis=1)
        score = mm(lhs, rhs)
        peak = jnp.max(score, axis=0, keepdims=True)
        return jnp.exp(score - peak).astype(BF16), peak

    def summed(t, p, first, count, weight):
        at = pl.ds(pl.multiple_of(p * 2 * HD + first, HD), count)
        lhs = jnp.concatenate([vals[at, pl.ds(t * frame_rows, frame_rows)], ones_rows], axis=0)
        return mm(lhs, weight)

    def store_part(s, h, context, total, peak):
        part[s, h, pl.ds(0, HD), :] = context
        eight = iota((8, tokens), 0)
        part[s, h, pl.ds(HD, 8), :] = jnp.where(eight == 0, total, peak)

    def pair_copy(p):
        two = pl.ds(2 * p, 2)
        return remote(part.at[other, two], pair_in.at[two], pc_s.at[p], pc_r.at[p], {"c": other})

    def one_pair(p, carry):
        first = (2 * HD * p) // chunk
        base = chunk * first - 2 * HD * p
        inner = sel_lane & (CP - 1)
        dim = base + chunk * (sel_lane >> 4) + inner
        pick = jnp.where((dim == sel_row) & (inner < chunk), HD**-0.5, 0.0).astype(BF16)
        q_rows = grid_q[pl.ds(first, NB)].reshape(NB * CP, steps * tokens)
        q_two = mm(pick, q_rows)
        rhs = [
            jnp.concatenate([jnp.where((row < HD) == (i == 0), q_two, 0.0).astype(BF16), unit], axis=0)
            for i in range(2)
        ]
        rhs_late = jnp.concatenate([r[:, tokens:] for r in rhs], axis=1)
        w_late, top_late = weigh(1, p, rhs_late)
        late = summed(1, p, 0, 2 * HD, w_late)
        for i in range(2):
            h = 2 * p + i
            w_old, top_old = weigh(0, p, rhs[i])
            old = summed(0, p, i * HD, HD, w_old)
            lanes = slice(i * tokens, (i + 1) * tokens)
            store_part(
                0, h, old[:HD, :tokens], old[HD : HD + 8, :tokens], top_old[:, :tokens] - slope[h] * dist[0]
            )
            peak_a = top_old[:, tokens:] - slope[h] * (dist[1] + 1.0)
            peak_b = top_late[:, lanes] - slope[h] * dist[1]
            peak = jnp.maximum(peak_a, peak_b)
            fa, fb = jnp.exp(peak_a - peak), jnp.exp(peak_b - peak)
            store_part(
                1,
                h,
                fa * old[:HD, tokens:] + fb * late[i * HD : (i + 1) * HD, lanes],
                fa * old[HD : HD + 8, tokens:] + fb * late[2 * HD : 2 * HD + 8, lanes],
                peak,
            )
        pair_copy(p).start()
        return carry

    lax.fori_loop(0, pairs, one_pair, 0)

    def x_copy(h):
        i, xx = h // nx, lax.rem(h, nx)
        return remote(xs.at[h], xr.at[x, i], x_s.at[h], x_r.at[x, i], {"x": xx})

    def merge_pair(p, carry):
        two = pl.ds(2 * p, 2)
        remote(part.at[other, two], pair_in.at[two], pc_s.at[p], pc_r.at[p], {"c": other}).wait_recv()
        for i in range(2):
            h = 2 * p + i
            mine, theirs = part[c, h], pair_in[h]
            peak_a, peak_b = mine[HD + 1 : HD + 2], theirs[HD + 1 : HD + 2]
            peak = jnp.maximum(peak_a, peak_b)
            fa, fb = jnp.exp(peak_a - peak), jnp.exp(peak_b - peak)
            merged = fa * mine[:HD] + fb * theirs[:HD]
            total = fa * mine[HD : HD + 1] + fb * theirs[HD : HD + 1]
            message = jnp.concatenate([merged, stats_tile(peak, total, 16)], axis=0).astype(BF16)

            @pl.when(lax.rem(h, nx) == x)
            def _():
                xr[x, h // nx] = message

            @pl.when(lax.rem(h, nx) != x)
            def _():
                xs[h] = message
                x_copy(h).start()

        return carry

    lax.fori_loop(0, pairs, merge_pair, 0)

    blocks, notes = [], []
    for i in range(hpx):
        for d in range(1, nx):
            xx = lax.rem(x + d, nx)
            remote(xs.at[i], xr.at[xx, i], x_s.at[i], x_r.at[xx, i], {"x": xx}).wait_recv()
        got = [xr[k, i].astype(F32) for k in range(nx)]
        peaks = [g[HD : HD + 1] + g[HD + 1 : HD + 2] + g[HD + 2 : HD + 3] for g in got]
        peak = functools.reduce(jnp.maximum, peaks)
        factors = [jnp.exp(one - peak) for one in peaks]
        blocks.append(sum(f * g[:HD] for f, g in zip(factors, got)))
        total = sum(f * (g[HD + 3 : HD + 4] + g[HD + 4 : HD + 5]) for f, g in zip(factors, got))
        notes.append(stats_tile(peak, total, 8))
    spare = span - hpx * (HD + 8)
    if spare:
        notes.append(jnp.zeros((spare, tokens), F32))
    by_token = jnp.concatenate(blocks + notes, axis=0).T
    zs[...] = by_token.reshape(nz, per_z, span).astype(BF16)
    zr[z] = zs[z]

    for d in far:
        zz = lax.rem(z + d, nz)
        remote(zs.at[zz], zr.at[z], z_s.at[d], z_r.at[z], {"z": zz}).start()
    for d in near:
        zz = lax.rem(z + d, nz)
        remote(zs.at[zz], zr.at[zz], z_s.at[d], z_r.at[zz], {"z": zz}).wait_recv()
    wide = zr[...].astype(F32)
    flat = wide.reshape(tokens, span).astype(BF16)
    from_row = iota((span, span), 0)
    to_lane = iota((span, span), 1)
    offset = from_row - slots - 8 * (to_lane >> 6)
    kept = to_lane < slots
    peak_of = jnp.where(kept & (offset >= 0) & (offset < 3), 1.0, 0.0).astype(BF16)
    total_of = jnp.where(kept & (offset >= 3) & (offset < 5), 1.0, 0.0).astype(BF16)
    peaks = mm(flat, peak_of).reshape(nz, per_z, span)
    totals = mm(flat, total_of).reshape(nz, per_z, span)
    factors = jnp.exp(peaks - jnp.max(peaks, axis=0, keepdims=True))
    context = jnp.sum(factors * wide, axis=0) / jnp.sum(factors * totals, axis=0)
    context = jnp.where(iota((per_z, span), 1) < slots, context, 0.0)
    ctx[x, z] = context.astype(BF16)

    for d in far:
        here = ctx.at[x, z]
        remote(here, here, g_s.at[d], g_r.at[z], {"z": lax.rem(z + d, nz)}).start()
    for d in [0] + near:
        zz = lax.rem(z + d, nz)
        here = ctx.at[x, zz]
        if d:
            remote(here, here, g_s.at[d], g_r.at[zz], {"z": zz}).wait_recv()
        for e in range(1, nx):
            remote(here, here, h_s.at[zz, e], h_r.at[zz, x], {"x": lax.rem(x + e, nx)}).start()
    for d in [0] + near:
        zz = lax.rem(z + d, nz)
        for e in range(1, nx):
            xx = lax.rem(x + e, nx)
            there = ctx.at[xx, zz]
            remote(there, there, h_s.at[zz, e], h_r.at[zz, xx], {"x": xx}).wait_recv()
    result = jnp.zeros((2 * CP, tokens), F32)
    for xx in range(nx):
        rows = ctx[xx].astype(F32).reshape(tokens, span).astype(BF16)
        result += mm_t(wo_all[xx], rows)
    o_out[...] = result[CP:].astype(BF16)
    swap = remote(o_out, o_in, o_s, o_r, {"c": other})
    swap.start()
    mine = result[:chunk]

    for d in near:
        zz = lax.rem(z + d, nz)
        q_over_z(d, zz).wait_send()
        remote(zs.at[zz], zr.at[z], z_s.at[d], z_r.at[z], {"z": zz}).wait_send()
        remote(ctx.at[x, z], ctx.at[x, z], g_s.at[d], g_r.at[z], {"z": zz}).wait_send()

    def close_z(zz, carry):
        for e in range(1, nx):
            q_over_x(zz, e).wait_send()
            here = ctx.at[x, zz]
            remote(here, here, h_s.at[zz, e], h_r.at[zz, x], {"x": lax.rem(x + e, nx)}).wait_send()
        for xx in range(nx):
            q_over_c(zz, xx).wait_send()
        return carry

    lax.fori_loop(0, nz, close_z, 0)

    def close_pair(p, carry):
        pair_copy(p).wait_send()
        for i in range(2):
            h = 2 * p + i

            @pl.when(lax.rem(h, nx) != x)
            def _():
                x_copy(h).wait_send()

        return carry

    lax.fori_loop(0, pairs, close_pair, 0)
    to_partner.wait_send()
    swap.wait()
    theirs = o_in[...].astype(F32)[:chunk]
    both = [jnp.where(c == 0, mine, theirs), jnp.where(c == 0, theirs, mine)]
    out[...] = jnp.stack(both, axis=1).astype(BF16)


def local(frames, dec_states, w_query, w_keyval, w_output, head_slope, lengths, positions):
    nz, nx, nc = (lax.axis_size(a) for a in SEQ)
    steps, frame_rows, width = frames.shape
    tokens = dec_states.shape[1]
    heads = head_slope.shape[0]
    chunk = w_query.shape[1]
    n = nz * nx * nc
    hpx = heads // nx
    span = -(-hpx * (HD + 8) // 128) * 128
    per_z = tokens // nz
    tall = steps * frame_rows
    sizes = (nz, nx, nc, steps, frame_rows, tokens, width, heads, chunk)
    vmem = pl.BlockSpec(memory_space=pltpu.VMEM)
    smem = pl.BlockSpec(memory_space=pltpu.SMEM)
    dma = pltpu.SemaphoreType.DMA
    flops = 2 * tall * width * 2 * width
    out = pl.pallas_call(
        functools.partial(kernel, sizes),
        out_shape=jax.ShapeDtypeStruct((chunk, steps, tokens), BF16),
        in_specs=[pl.BlockSpec(memory_space=pl.ANY)] * 2 + [vmem] * 4 + [smem] * 2,
        out_specs=vmem,
        scratch_shapes=[
            pltpu.VMEM((tall, width), BF16),
            pltpu.VMEM((width, 2 * width), BF16),
            pltpu.VMEM((tall, width), BF16),
            pltpu.VMEM((width, tall), BF16),
            pltpu.VMEM((steps, frame_rows, 128), BF16),
            pltpu.VMEM((n + NB, CP, steps * tokens), BF16),
            pltpu.VMEM((CP, steps * tokens), F32),
            pltpu.VMEM((steps, heads, HD + 8, tokens), F32),
            pltpu.VMEM((heads, HD + 8, tokens), F32),
            pltpu.VMEM((heads, HD + 16, tokens), BF16),
            pltpu.VMEM((nx, hpx, HD + 16, tokens), BF16),
            pltpu.VMEM((nz, per_z, span), BF16),
            pltpu.VMEM((nz, per_z, span), BF16),
            pltpu.VMEM((nx, nz, per_z, span), BF16),
            pltpu.VMEM((chunk, width), BF16),
            pltpu.VMEM((nx, 2 * CP, span), BF16),
            pltpu.VMEM((CP, tokens), BF16),
            pltpu.VMEM((CP, tokens), BF16),
            dma((tall // ROWS,)),
            dma((2 * width // COLS,)),
            dma((nz,)),
            dma((nz,)),
            dma((nz, nx)),
            dma((nz, nx)),
            dma((nz, nx)),
            dma((nz, nx)),
            dma,
            dma,
            dma((heads // 2,)),
            dma((heads // 2,)),
            dma((heads,)),
            dma((nx, hpx)),
            dma((nz,)),
            dma((nz,)),
            dma((nz,)),
            dma((nz,)),
            dma((nz, nx)),
            dma((nz, nx)),
            dma,
            dma,
        ],
        compiler_params=pltpu.CompilerParams(
            collective_id=0, has_side_effects=True, vmem_limit_bytes=60 * 1024 * 1024
        ),
        cost_estimate=pl.CostEstimate(flops=flops, bytes_accessed=2 * width * (tall + 2 * width), transcendentals=0),
        name="attend",
    )(frames.reshape(tall, width), w_keyval, dec_states.reshape(steps * tokens, width), w_query.T, w_output.T,
      positions, lengths, head_slope)
    return out.transpose(1, 2, 0)


def solution(mesh):
    devices = mesh.devices.reshape(mesh.shape["grp"], 16, 4, 2)
    finer = Mesh(devices, ("grp",) + SEQ)
    return jax.shard_map(
        local,
        mesh=finer,
        in_specs=(
            P("grp", SEQ, None),
            P(None, "grp", None),
            P(None, SEQ),
            P(),
            P(None, SEQ),
            P(),
            P("grp", None),
            P(None, "grp"),
        ),
        out_specs=P(None, "grp", SEQ),
        check_vma=False,
    )
```

```python
import functools

import jax
import jax.numpy as jnp
from jax import lax
from jax.experimental import pallas as pl
from jax.experimental.pallas import tpu as pltpu
from jax.sharding import Mesh
from jax.sharding import PartitionSpec as P

SEQ = ("z", "x", "c")
F32, BF16 = jnp.float32, jnp.bfloat16
HD = 64
CP = 16
NB = 16
COLS = 256
LOW = -1e30


def mm(a, b):
    return jnp.dot(a, b, preferred_element_type=F32)


def mm_t(a, b):
    return lax.dot_general(a, b, (((1,), (1,)), ((), ())), preferred_element_type=F32)


def iota(shape, dim):
    return lax.broadcasted_iota(jnp.int32, shape, dim)


def remote(src, dst, send, recv, device):
    return pltpu.make_async_remote_copy(
        src_ref=src,
        dst_ref=dst,
        send_sem=send,
        recv_sem=recv,
        device_id=device,
        device_id_type=pl.DeviceIdType.MESH,
    )


def near_first(n):
    order = []
    for d in range(1, n // 2 + 1):
        order.append(d)
        if n - d != d:
            order.append(n - d)
    return order


def pieces(value, count):
    parts = []
    for _ in range(count):
        part = value.astype(BF16).astype(F32)
        parts.append(part)
        value = value - part
    return parts


def stats_tile(peak, total, rows):
    at = iota((rows, peak.shape[-1]), 0)
    tile = jnp.zeros((rows, peak.shape[-1]), F32)
    for k, part in enumerate(pieces(peak, 3) + pieces(total, 2)):
        tile = jnp.where(at == k, part, tile)
    return tile


def kernel(
    sizes,
    frames, wkv, dec, wq, wo, pos, lens, slope,
    out,
    fr, wt, dec_v, wq_v, wo_v, keys, vals, mask, grid_q, qpad, rhs_v, score_v, weight_v, part, pair_in, xs, xr, zs, zr, ctx,
    wo_rows, wo_all, fin_out, fin_in,
    fr_sem, wt_sem, in_sem, qz_s, qz_r, qx_s, qx_r, qc_s, qc_r, wo_s, wo_r, pc_s, pc_r, x_s, x_r, z_s, z_r, g_s, g_r, f_s, f_r,
):
    nz, nx, nc, steps, frame_rows, tokens, width, heads, chunk = sizes
    n = nz * nx * nc
    z, x, c = lax.axis_index("z"), lax.axis_index("x"), lax.axis_index("c")
    row_size = nx * nc
    mine = x * nc + c
    own = z * row_size + mine
    other = 1 - c
    near = near_first(nz)
    far = near[::-1]
    reach = nz // 4
    hpx = heads // nx
    pairs = heads // 2
    per_group = nx // 2
    slots = hpx * HD
    span = zs.shape[-1]
    per_z = tokens // nz
    tall = steps * frame_rows
    tiles = 2 * width // COLS
    mesh_id = pl.DeviceIdType.MESH

    def along(d):
        return lax.rem(z + d + nz, nz)

    def row_peer(r):
        t = lax.rem(mine + r, row_size)
        return t, {"x": t // nc, "c": lax.rem(t, nc)}

    barrier = pltpu.get_barrier_semaphore()
    close = [k for d in range(1, reach + 1) for k in (d, -d)]
    for d in close[::-1]:
        pl.semaphore_signal(barrier, inc=1, device_id={"z": along(d)}, device_id_type=mesh_id)
    for r in range(1, row_size):
        pl.semaphore_signal(barrier, inc=1, device_id=row_peer(r)[1], device_id_type=mesh_id)

    small = [
        pltpu.make_async_copy(src, dst, in_sem.at[k]) for k, (src, dst) in enumerate(((dec, dec_v), (wq, wq_v), (wo, wo_v)))
    ]
    loads = [
        pltpu.make_async_copy(frames.at[pl.ds(k * frame_rows, frame_rows), :], fr.at[pl.ds(k * frame_rows, frame_rows), :], fr_sem.at[k])
        for k in range(steps)
    ]

    def tile_load(j):
        cols = pl.ds(pl.multiple_of(j * COLS, COLS), COLS)
        return pltpu.make_async_copy(wkv.at[:, cols], wt.at[:, cols], wt_sem.at[j])

    for load in small + loads:
        load.start()
    tile_load(0).start()

    grid_q[pl.ds(n, NB)] = jnp.zeros((NB, CP, steps * tokens), BF16)
    qpad[...] = jnp.zeros_like(qpad)
    small[0].wait()
    small[1].wait()
    qpad[:chunk] = mm_t(wq_v[...], dec_v[...])
    grid_q[own] = qpad[...].astype(BF16)
    small[2].wait()
    wo_rows[mine] = jnp.zeros((CP, width), BF16)
    wo_rows[mine, :chunk, :] = wo_v[...]

    pl.semaphore_wait(barrier, len(close) + row_size - 1)

    def q_chunk(zz, xx, cc):
        return grid_q.at[zz * row_size + xx * nc + cc]

    def q_over_z(k, source, d):
        here = q_chunk(source, x, c)
        return remote(here, here, qz_s.at[k], qz_r.at[source], {"z": along(d)})

    def q_over_x(zz, d):
        here = q_chunk(zz, x, c)
        return remote(here, here, qx_s.at[zz, d], qx_r.at[zz, x], {"x": lax.rem(x + d, nx)})

    def q_over_c(zz, xx):
        here = q_chunk(zz, xx, c)
        return remote(here, here, qc_s.at[zz, xx], qc_r.at[zz, xx], {"c": other})

    first_stage = [(k, z, d) for k, d in enumerate(close[::-1])]
    second_stage = [(len(close) + d - 1, along(-reach), d) for d in range(reach, 0, -1)]
    second_stage += [(len(close) + reach + d - 1, along(reach), -d) for d in range(reach - 1, 0, -1)]
    for args in first_stage:
        q_over_z(*args).start()

    def wo_over_row(r):
        return remote(wo_rows.at[mine], wo_rows.at[mine], wo_s.at[r], wo_r.at[mine], row_peer(r)[1])

    def spread(zz):
        for e in range(1, nx):
            q_over_x(zz, e).start()
        q_over_c(zz, x).start()

    spread(z)

    def arrive_z(zz):
        here = q_chunk(zz, x, c)
        remote(here, here, qz_s.at[0], qz_r.at[zz], {"z": zz}).wait_recv()

    def relay():
        arrive_z(along(-reach))
        arrive_z(along(reach))
        for args in second_stage:
            q_over_z(*args).start()
        for r in range(1, row_size):
            wo_over_row(r).start()

    def spread_near():
        for d in close:
            if abs(d) < reach:
                arrive_z(along(d))
            spread(along(d))

    distant = [d for k in range(reach + 1, nz // 2 + 1) for d in ((k, -k) if 2 * k < nz else (k,))]

    def spread_far():
        for d in distant:
            arrive_z(along(d))
            spread(along(d))

    def cross(ds):
        for d in ds:
            zz = along(d)
            for e in range(1, nx):
                xx = lax.rem(x + e, nx)
                here = q_chunk(zz, xx, c)
                remote(here, here, qx_s.at[zz, e], qx_r.at[zz, xx], {"x": xx}).wait_recv()
                q_over_c(zz, xx).start()

    at_lane = iota((frame_rows, 128), 1)
    at_row = iota((frame_rows, 128), 0)
    for t in range(steps):
        hidden = (at_lane == 0) & (at_row >= lens[t, own])
        mask[t] = jnp.where(hidden, LOW, 0.0).astype(BF16)
    for load in loads:
        load.wait()
    for j in range(1, tiles):
        tile_load(j).start()

    half = tiles // 2

    def project_keys(j, carry):
        tile_load(j).wait()
        cols = pl.ds(pl.multiple_of(j * COLS, COLS), COLS)
        keys[:, cols] = mm(fr[...], wt[:, cols]).astype(BF16)

        @pl.when(j == (half - 1) // 2)
        def _():
            relay()

        @pl.when(j == half - 1)
        def _():
            spread_near()

        return carry

    def project_values(j, carry):
        tile_load(j + half).wait()
        cols = pl.ds(pl.multiple_of(j * COLS + width, COLS), COLS)
        head_rows = pl.ds(pl.multiple_of(j * COLS, COLS), COLS)
        vals[head_rows, :] = mm(fr[...], wt[:, cols]).astype(BF16).T

        @pl.when(j == half // 2 - 1 if half > 1 else j == 0)
        def _():
            spread_far()

        @pl.when(j == half - 2 if half > 1 else j == 0)
        def _():
            cross([0] + close)

        return carry

    lax.fori_loop(0, half, project_keys, 0)
    lax.fori_loop(0, half, project_values, 0)
    cross(distant)

    for r in range(1, row_size):
        t, peer = row_peer(r)
        remote(wo_rows.at[t], wo_rows.at[t], wo_s.at[r], wo_r.at[t], peer).wait_recv()
    lane = iota((width, span), 1)
    source = ((lane >> 6) * nx + x) * HD + (lane & (HD - 1))
    take = jnp.where((iota((width, span), 0) == source) & (lane < slots), 1.0, 0.0).astype(BF16)
    wo_all[...] = mm(wo_rows[...].reshape(row_size * CP, width), take).astype(BF16)

    place = lax.rem(own + 1, n).astype(F32)
    dist = [jnp.abs(pos[pl.ds(s, 1), :].astype(F32) - place) / n for s in range(steps)]
    ones_rows = jnp.ones((16, frame_rows), BF16)
    row = iota((2 * HD, steps * tokens), 0)
    unit = jnp.where(row == 0, 1.0, 0.0).astype(BF16)
    jobs = ((0, 0), (0, 1), (1, None))
    tops = {}
    crossed = [0]

    def prepare(p):
        first = (2 * HD * p) // chunk
        while crossed[0] < min(nz, (first + NB - 1) // row_size + 1):
            for xx in range(nx):
                here = q_chunk(crossed[0], xx, other)
                remote(here, here, qc_s.at[0, 0], qc_r.at[crossed[0], xx], {"c": other}).wait_recv()
            crossed[0] += 1
        sel_lane = iota((2 * HD, NB * CP), 1)
        inner = sel_lane & (CP - 1)
        dim = chunk * first - 2 * HD * p + chunk * (sel_lane >> 4) + inner
        pick = jnp.where((dim == iota((2 * HD, NB * CP), 0)) & (inner < chunk), HD**-0.5, 0.0).astype(BF16)
        q_two = mm(pick, grid_q[pl.ds(first, NB)].reshape(NB * CP, steps * tokens))
        rhs = [
            jnp.concatenate([jnp.where((row < HD) == (i == 0), q_two, 0.0).astype(BF16), unit], axis=0)
            for i in range(2)
        ]
        rhs.append(jnp.concatenate([r[:, tokens:] for r in rhs], axis=1))
        for k in range(3):
            rhs_v[p % 2, k] = rhs[k]

    def scores(p):
        for k, (t, _) in enumerate(jobs):
            lhs = jnp.concatenate([keys[pl.ds(t * frame_rows, frame_rows), pl.ds(p * 2 * HD, 2 * HD)], mask[t]], axis=1)
            score = mm(lhs, rhs_v[p % 2, k])
            score_v[p % 2, k] = score
            tops[p, k] = jnp.max(score, axis=0, keepdims=True)

    def weights(p):
        for k in range(3):
            weight_v[p % 2, k] = jnp.exp(score_v[p % 2, k] - tops[p, k]).astype(BF16)

    def store_part(s, h, context, total, peak):
        part[s, h, pl.ds(0, HD), :] = context
        part[s, h, pl.ds(HD, 8), :] = jnp.where(iota((8, tokens), 0) == 0, total, peak)

    def sums(p):
        result = []
        for k, (t, i) in enumerate(jobs):
            at = pl.ds(p * 2 * HD + (i or 0) * HD, 2 * HD if i is None else HD)
            lhs = jnp.concatenate([vals[at, pl.ds(t * frame_rows, frame_rows)], ones_rows], axis=0)
            result.append(mm(lhs, weight_v[p % 2, k]))
        late = result[2]
        for i in range(2):
            h = 2 * p + i
            old, top_old = result[i], tops[p, i]
            lanes = slice(i * tokens, (i + 1) * tokens)
            store_part(0, h, old[:HD, :tokens], old[HD : HD + 8, :tokens], top_old[:, :tokens] - slope[h] * dist[0])
            peak_a = top_old[:, tokens:] - slope[h] * (dist[1] + 1.0)
            peak_b = tops[p, 2][:, lanes] - slope[h] * dist[1]
            peak = jnp.maximum(peak_a, peak_b)
            fa, fb = jnp.exp(peak_a - peak), jnp.exp(peak_b - peak)
            store_part(
                1,
                h,
                fa * old[:HD, tokens:] + fb * late[i * HD : (i + 1) * HD, lanes],
                fa * old[HD : HD + 8, tokens:] + fb * late[2 * HD : 2 * HD + 8, lanes],
                peak,
            )

    def pair_copy(p):
        two = pl.ds(2 * p, 2)
        return remote(part.at[other, two], pair_in.at[two], pc_s.at[p], pc_r.at[p], {"c": other})

    def x_copy(i, e):
        xx = lax.rem(x + e, nx)
        return remote(xs.at[i * nx + xx], xr.at[i, x], x_s.at[i, e], x_r.at[i, x], {"x": xx})

    def merge_group(i):
        for p in range(i * per_group, (i + 1) * per_group):
            pair_copy(p).wait_recv()
        for h in range(i * nx, (i + 1) * nx):
            own_part, their_part = part[c, h], pair_in[h]
            peak_a, peak_b = own_part[HD + 1 : HD + 2], their_part[HD + 1 : HD + 2]
            peak = jnp.maximum(peak_a, peak_b)
            fa, fb = jnp.exp(peak_a - peak), jnp.exp(peak_b - peak)
            merged = fa * own_part[:HD] + fb * their_part[:HD]
            total = fa * own_part[HD : HD + 1] + fb * their_part[HD : HD + 1]
            xs[h] = jnp.concatenate([merged, stats_tile(peak, total, 16)], axis=0).astype(BF16)
        for e in range(1, nx):
            x_copy(i, e).start()

    blocks, notes = {}, {}

    def gather_group(i):
        got = [xs[i * nx + x].astype(F32)]
        for e in range(1, nx):
            xx = lax.rem(x + e, nx)
            remote(xs.at[i], xr.at[i, xx], x_s.at[i, e], x_r.at[i, xx], {"x": xx}).wait_recv()
        for e in range(1, nx):
            got.append(xr[i, lax.rem(x + e, nx)].astype(F32))
        peaks = [g[HD : HD + 1] + g[HD + 1 : HD + 2] + g[HD + 2 : HD + 3] for g in got]
        peak = functools.reduce(jnp.maximum, peaks)
        factors = [jnp.exp(one - peak) for one in peaks]
        blocks[i] = sum(f * g[:HD] for f, g in zip(factors, got))
        total = sum(f * (g[HD + 3 : HD + 4] + g[HD + 4 : HD + 5]) for f, g in zip(factors, got))
        notes[i] = stats_tile(peak, total, 8)

    merged = gathered = 0
    for it in range(pairs + 3):
        if it < pairs:
            prepare(it)
        if 0 <= it - 1 < pairs:
            scores(it - 1)
        if 0 <= it - 2 < pairs:
            weights(it - 2)
        if 0 <= it - 3 < pairs:
            sums(it - 3)
            pair_copy(it - 3).start()
        if merged < hpx and it - 3 >= (merged + 1) * per_group - 1 + 2:
            merge_group(merged)
            merged += 1
    while merged < hpx:
        merge_group(merged)
        merged += 1
    while gathered < hpx:
        gather_group(gathered)
        gathered += 1
    filled = [blocks[i] for i in range(hpx)] + [notes[i] for i in range(hpx)]
    spare = span - hpx * (HD + 8)
    if spare:
        filled.append(jnp.zeros((spare, tokens), F32))
    by_token = jnp.concatenate(filled, axis=0).T
    zs[...] = by_token.reshape(nz, per_z, span).astype(BF16)
    zr[z] = zs[z]

    def z_copy(d):
        zz = along(d)
        return remote(zs.at[zz], zr.at[z], z_s.at[d], z_r.at[z], {"z": zz})

    for d in far:
        z_copy(d).start()
    for d in near:
        zz = along(d)
        remote(zs.at[zz], zr.at[zz], z_s.at[d], z_r.at[zz], {"z": zz}).wait_recv()
    wide = zr[...].astype(F32)
    flat = wide.reshape(tokens, span).astype(BF16)
    to_lane = iota((span, span), 1)
    offset = iota((span, span), 0) - slots - 8 * (to_lane >> 6)
    kept = to_lane < slots
    peak_of = jnp.where(kept & (offset >= 0) & (offset < 3), 1.0, 0.0).astype(BF16)
    total_of = jnp.where(kept & (offset >= 3) & (offset < 5), 1.0, 0.0).astype(BF16)
    peaks = mm(flat, peak_of).reshape(nz, per_z, span)
    totals = mm(flat, total_of).reshape(nz, per_z, span)
    factors = jnp.exp(peaks - jnp.max(peaks, axis=0, keepdims=True))
    context = jnp.sum(factors * wide, axis=0) / jnp.sum(factors * totals, axis=0)
    context = jnp.where(iota((per_z, span), 1) < slots, context, 0.0)
    ctx[z] = context.astype(BF16)

    def g_copy(d):
        return remote(ctx.at[z], ctx.at[z], g_s.at[d], g_r.at[z], {"z": along(d)})

    for d in far:
        g_copy(d).start()
    for d in near:
        zz = along(d)
        remote(ctx.at[zz], ctx.at[zz], g_s.at[d], g_r.at[zz], {"z": zz}).wait_recv()

    rows = ctx[...].astype(F32).reshape(tokens, span).astype(BF16)
    fin_out[...] = mm_t(wo_all[...], rows).reshape(row_size, CP, tokens)

    def f_copy(r):
        t, peer = row_peer(r)
        return remote(fin_out.at[t], fin_in.at[mine], f_s.at[r], f_r.at[mine], peer)

    for r in range(1, row_size):
        f_copy(r).start()
    fin_in[mine] = fin_out[mine]

    for args in first_stage + second_stage:
        q_over_z(*args).wait_send()
    for d in near:
        z_copy(d).wait_send()
        g_copy(d).wait_send()
    for r in range(1, row_size):
        wo_over_row(r).wait_send()

    def close_z(zz, carry):
        for e in range(1, nx):
            q_over_x(zz, e).wait_send()
        for xx in range(nx):
            q_over_c(zz, xx).wait_send()
        return carry

    lax.fori_loop(0, nz, close_z, 0)
    for p in range(pairs):
        pair_copy(p).wait_send()
    for i in range(hpx):
        for e in range(1, nx):
            x_copy(i, e).wait_send()
    for r in range(1, row_size):
        t, peer = row_peer(r)
        remote(fin_out.at[t], fin_in.at[t], f_s.at[r], f_r.at[t], peer).wait_recv()
    both = [sum(fin_in[xx * nc + s] for xx in range(nx))[:chunk] for s in range(steps)]
    out[...] = jnp.stack(both, axis=1).astype(BF16)
    for r in range(1, row_size):
        f_copy(r).wait_send()


def local(frames, dec_states, w_query, w_keyval, w_output, head_slope, lengths, positions):
    nz, nx, nc = (lax.axis_size(a) for a in SEQ)
    steps, frame_rows, width = frames.shape
    tokens = dec_states.shape[1]
    heads = head_slope.shape[0]
    chunk = w_query.shape[1]
    n = nz * nx * nc
    hpx = heads // nx
    span = -(-hpx * (HD + 8) // 128) * 128
    per_z = tokens // nz
    tall = steps * frame_rows
    row_size = nx * nc
    sizes = (nz, nx, nc, steps, frame_rows, tokens, width, heads, chunk)
    vmem = pl.BlockSpec(memory_space=pltpu.VMEM)
    smem = pl.BlockSpec(memory_space=pltpu.SMEM)
    dma = pltpu.SemaphoreType.DMA
    flops = 2 * tall * width * 2 * width
    out = pl.pallas_call(
        functools.partial(kernel, sizes),
        out_shape=jax.ShapeDtypeStruct((chunk, steps, tokens), BF16),
        in_specs=[pl.BlockSpec(memory_space=pl.ANY)] * 5 + [vmem] + [smem] * 2,
        out_specs=vmem,
        scratch_shapes=[
            pltpu.VMEM((tall, width), BF16),
            pltpu.VMEM((width, 2 * width), BF16),
            pltpu.VMEM((steps * tokens, width), BF16),
            pltpu.VMEM((chunk, width), BF16),
            pltpu.VMEM((chunk, width), BF16),
            pltpu.VMEM((tall, width), BF16),
            pltpu.VMEM((width, tall), BF16),
            pltpu.VMEM((steps, frame_rows, 128), BF16),
            pltpu.VMEM((n + NB, CP, steps * tokens), BF16),
            pltpu.VMEM((CP, steps * tokens), F32),
            pltpu.VMEM((2, 3, 4 * HD, steps * tokens), BF16),
            pltpu.VMEM((2, 3, frame_rows, steps * tokens), F32),
            pltpu.VMEM((2, 3, frame_rows, steps * tokens), BF16),
            pltpu.VMEM((steps, heads, HD + 8, tokens), F32),
            pltpu.VMEM((heads, HD + 8, tokens), F32),
            pltpu.VMEM((heads, HD + 16, tokens), BF16),
            pltpu.VMEM((hpx, nx, HD + 16, tokens), BF16),
            pltpu.VMEM((nz, per_z, span), BF16),
            pltpu.VMEM((nz, per_z, span), BF16),
            pltpu.VMEM((nz, per_z, span), BF16),
            pltpu.VMEM((row_size, CP, width), BF16),
            pltpu.VMEM((row_size * CP, span), BF16),
            pltpu.VMEM((row_size, CP, tokens), F32),
            pltpu.VMEM((row_size, CP, tokens), F32),
            dma((steps,)),
            dma((2 * width // COLS,)),
            dma((3,)),
            dma((nz,)),
            dma((nz,)),
            dma((nz, nx)),
            dma((nz, nx)),
            dma((nz, nx)),
            dma((nz, nx)),
            dma((row_size,)),
            dma((row_size,)),
            dma((heads // 2,)),
            dma((heads // 2,)),
            dma((hpx, nx)),
            dma((hpx, nx)),
            dma((nz,)),
            dma((nz,)),
            dma((nz,)),
            dma((nz,)),
            dma((row_size,)),
            dma((row_size,)),
        ],
        compiler_params=pltpu.CompilerParams(
            collective_id=0, has_side_effects=True, vmem_limit_bytes=60 * 1024 * 1024
        ),
        cost_estimate=pl.CostEstimate(flops=flops, bytes_accessed=2 * width * (tall + 2 * width), transcendentals=0),
        name="attend",
    )(frames.reshape(tall, width), w_keyval, dec_states.reshape(steps * tokens, width), w_query.T, w_output.T,
      positions, lengths, head_slope)
    return out.transpose(1, 2, 0)


def solution(mesh):
    devices = mesh.devices.reshape(mesh.shape["grp"], 16, 4, 2)
    finer = Mesh(devices, ("grp",) + SEQ)
    return jax.shard_map(
        local,
        mesh=finer,
        in_specs=(
            P("grp", SEQ, None),
            P(None, "grp", None),
            P(None, SEQ),
            P(),
            P(None, SEQ),
            P(),
            P("grp", None),
            P(None, "grp"),
        ),
        out_specs=P(None, "grp", SEQ),
        check_vma=False,
    )
```

```python
import functools

import jax
import jax.numpy as jnp
from jax import lax
from jax.experimental import pallas as pl
from jax.experimental.pallas import tpu as pltpu
from jax.sharding import Mesh
from jax.sharding import PartitionSpec as P

SEQ = ("z", "x", "c")
F32, BF16 = jnp.float32, jnp.bfloat16
HD = 64
CP = 16
COLS = 256
LOW = -1e30


def mm(a, b):
    return jnp.dot(a, b, preferred_element_type=F32)


def mm_t(a, b):
    return lax.dot_general(a, b, (((1,), (1,)), ((), ())), preferred_element_type=F32)


def iota(shape, dim):
    return lax.broadcasted_iota(jnp.int32, shape, dim)


def remote(src, dst, send, recv, device):
    return pltpu.make_async_remote_copy(
        src_ref=src,
        dst_ref=dst,
        send_sem=send,
        recv_sem=recv,
        device_id=device,
        device_id_type=pl.DeviceIdType.MESH,
    )


def near_first(n):
    order = []
    for d in range(1, n // 2 + 1):
        order.append(d)
        if n - d != d:
            order.append(n - d)
    return order


def pieces(value, count):
    parts = []
    for _ in range(count):
        part = value.astype(BF16).astype(F32)
        parts.append(part)
        value = value - part
    return parts


def log2(k):
    assert k & (k - 1) == 0
    return k.bit_length() - 1


def window(p, chunk, row_size):
    return 2 * HD * p // chunk // row_size, (2 * HD * (p + 1) - 1) // chunk // row_size + 1


def z_stages(hpx):
    return [tuple(range(hpx))]


def stage_span(stage):
    return -(-len(stage) * (HD + 8) // 128) * 128


def stats_tile(peak, total, rows):
    at = iota((rows, peak.shape[-1]), 0)
    tile = jnp.zeros((rows, peak.shape[-1]), F32)
    for k, part in enumerate(pieces(peak, 3) + pieces(total, 2)):
        tile = jnp.where(at == k, part, tile)
    return tile


def kernel(
    sizes,
    frames, wkv, dec, wq, wo, pos, lens, slope,
    out,
    *scratch,
):
    nz, nx, nc, steps, frame_rows, tokens, width, heads, chunk = sizes
    n = nz * nx * nc
    z, x, c = lax.axis_index("z"), lax.axis_index("x"), lax.axis_index("c")
    row_size = nx * nc
    mine = x * nc + c
    own = z * row_size + mine
    other = 1 - c
    near = near_first(nz)
    far = near[::-1]
    reach = nz // 4
    hpx = heads // nx
    pairs = heads // 2
    per_group = nx // 2
    stages = z_stages(hpx)
    ns = len(stages)
    it_ = iter(scratch)
    fr, wt, dec_v, wq_v, wo_v, keys, vals, mask, grid_q, qpad, rhs_v, score_v, weight_v, part, pair_in, xs, xr, wo_rows, fin_out, fin_in = (
        next(it_) for _ in range(20)
    )
    zs, zr, ctx, wo_all = ([next(it_) for _ in stages] for _ in range(4))
    fr_sem, wt_sem, in_sem, qz_s, qz_r, qx_s, qx_r, qc_s, qc_r, wo_s, wo_r, pc_s, pc_r, x_s, x_r, z_s, z_r, g_s, g_r, f_s, f_r = it_
    per_z = tokens // nz
    tall = steps * frame_rows
    tiles = 2 * width // COLS
    mesh_id = pl.DeviceIdType.MESH

    def along(d):
        return lax.rem(z + d + nz, nz)

    def slot(zz, xx, cc):
        return (zz * nc + cc) * nx + xx

    def wait_all(ref, send=None, recv=None):
        if send is not None:
            remote(ref, ref, send, send, {"c": 1 - c}).wait_send()
        else:
            remote(ref, ref, recv, recv, {"c": 1 - c}).wait_recv()

    def row_peer(r):
        t = lax.rem(mine + r, row_size)
        return t, {"x": t // nc, "c": lax.rem(t, nc)}

    small = [
        pltpu.make_async_copy(src, dst, in_sem.at[k]) for k, (src, dst) in enumerate(((dec, dec_v), (wq, wq_v), (wo, wo_v)))
    ]
    loads = [
        pltpu.make_async_copy(frames.at[pl.ds(k * frame_rows, frame_rows), :], fr.at[pl.ds(k * frame_rows, frame_rows), :], fr_sem.at[k])
        for k in range(steps)
    ]

    def tile_load(j):
        cols = pl.ds(pl.multiple_of(j * COLS, COLS), COLS)
        return pltpu.make_async_copy(wkv.at[:, cols], wt.at[:, cols], wt_sem.at[j])

    for load in small + loads:
        load.start()
    tile_load(0).start()

    barrier = pltpu.get_barrier_semaphore()
    close = [k for d in range(1, reach + 1) for k in (d, -d)]
    for d in close[::-1]:
        pl.semaphore_signal(barrier, inc=1, device_id={"z": along(d)}, device_id_type=mesh_id)
    for r in range(1, row_size):
        pl.semaphore_signal(barrier, inc=1, device_id=row_peer(r)[1], device_id_type=mesh_id)

    qpad[...] = jnp.zeros_like(qpad)
    small[0].wait()
    small[1].wait()
    qpad[:chunk] = mm_t(wq_v[...], dec_v[...])
    grid_q[slot(z, x, c)] = qpad[...].astype(BF16)
    pl.semaphore_wait(barrier, len(close) + row_size - 1)

    def q_chunk(zz, xx, cc):
        return grid_q.at[slot(zz, xx, cc)]

    def q_over_z(source, d):
        here = q_chunk(source, x, c)
        return remote(here, here, qz_s, qz_r.at[source], {"z": along(d)})

    def q_over_x(zz, d):
        here = q_chunk(zz, x, c)
        return remote(here, here, qx_s, qx_r.at[zz], {"x": lax.rem(x + d, nx)})

    def q_over_c(zz, cc):
        here = grid_q.at[pl.ds(slot(zz, 0, cc), nx)]
        return remote(here, here, qc_s, qc_r.at[zz], {"c": other})

    first_stage = [(z, d) for d in close[::-1]]
    second_stage = [(along(-reach), d) for d in range(reach, 0, -1)]
    second_stage += [(along(reach), -d) for d in range(reach - 1, 0, -1)]
    for args in first_stage:
        q_over_z(*args).start()

    def wo_over_row(r):
        return remote(wo_rows.at[mine], wo_rows.at[mine], wo_s, wo_r, row_peer(r)[1])

    def spread(zz):
        for e in range(1, nx):
            q_over_x(zz, e).start()

    def arrive_z(zz):
        here = q_chunk(zz, x, c)
        wait_all(here, recv=qz_r.at[zz])

    def relay():
        arrive_z(along(-reach))
        arrive_z(along(reach))
        for args in second_stage:
            q_over_z(*args).start()
        for d in (-reach, reach):
            spread(along(d))

    def spread_near():
        for d in close:
            if abs(d) < reach:
                arrive_z(along(d))
                spread(along(d))

    distant = [*range(reach + 1, nz // 2), *range(-nz // 2 + 1, -reach), nz // 2]

    def spread_far():
        for d in distant:
            arrive_z(along(d))
            spread(along(d))

    crossed = [0, 0]

    def cross_rows(after):
        for zz in range(crossed[0], after):
            wait_all(grid_q.at[pl.ds(0, nx - 1)], recv=qx_r.at[zz])
            q_over_c(zz, c).start()
        crossed[0] = max(crossed[0], after)

    spread(z)
    small[2].wait()
    wo_rows[mine] = jnp.zeros((CP, width), BF16)
    wo_rows[mine, :chunk, :] = wo_v[...]
    for r in range(1, row_size):
        wo_over_row(r).start()

    at_lane = iota((frame_rows, 128), 1)
    at_row = iota((frame_rows, 128), 0)
    for t in range(steps):
        hidden = (at_lane == 0) & (at_row >= lens[t, own])
        mask[t] = jnp.where(hidden, LOW, 0.0).astype(BF16)
    loads[0].wait()
    tile_load(0).wait()
    for j in range(1, tiles):
        tile_load(j).start()

    for t in range(steps):
        if t:
            loads[t].wait()
        rows = pl.ds(t * frame_rows, frame_rows)
        keys[rows, :COLS] = mm(fr[rows, :], wt[:, :COLS]).astype(BF16)
    half = tiles // 2

    def project_keys(j, carry):
        tile_load(j).wait()
        cols = pl.ds(pl.multiple_of(j * COLS, COLS), COLS)
        keys[:, cols] = mm(fr[...], wt[:, cols]).astype(BF16)

        @pl.when(j == max(half // 2, 1))
        def _():
            spread_near()

        @pl.when(j == max(half - 2, 1))
        def _():
            relay()

        return carry

    def project_values(j, carry):
        tile_load(j + half).wait()
        cols = pl.ds(pl.multiple_of(j * COLS + width, COLS), COLS)
        head_rows = pl.ds(pl.multiple_of(j * COLS, COLS), COLS)
        vals[head_rows, :] = mm(fr[...], wt[:, cols]).astype(BF16).T

        @pl.when(j == min(half // 2 - 1, half - 2))
        def _():
            spread_far()

        @pl.when(j == half - 2)
        def _():
            cross_rows(window(per_group - 1, chunk, row_size)[1])

        return carry

    lax.fori_loop(1, half, project_keys, 0)
    lax.fori_loop(0, half, project_values, 0)

    place = lax.rem(own + 1, n).astype(F32)
    dist = [jnp.abs(pos[pl.ds(s, 1), :].astype(F32) - place) / n for s in range(steps)]
    ones_rows = jnp.ones((16, frame_rows), BF16)
    row = iota((2 * HD, steps * tokens), 0)
    unit = jnp.where(row == 0, 1.0, 0.0).astype(BF16)
    jobs = ((0, 0), (0, 1), (1, None))
    tops = {}
    def prepare(p):
        first, after = window(p, chunk, row_size)
        if p % per_group == 0:
            cross_rows(window(min(p + 2 * per_group, pairs) - 1, chunk, row_size)[1])
            last = window(p + per_group - 1, chunk, row_size)[1]
            for zz in range(crossed[1], last):
                wait_all(grid_q.at[pl.ds(0, nx)], recv=qc_r.at[zz])
            crossed[1] = max(crossed[1], last)
        depth = (after - first) * row_size * CP
        at = iota((1, depth), 1)
        inner = at & (CP - 1)
        number = at >> log2(CP)
        in_row = ((number & (nx - 1)) << log2(nc)) + ((number >> log2(nx)) & (nc - 1))
        device = first * row_size + (number & -row_size) + in_row
        dim = jnp.where(inner < chunk, chunk * device + inner - 2 * HD * p, -1)
        pick = jnp.where(iota((2 * HD, depth), 0) == dim, HD**-0.5, 0.0).astype(BF16)
        q_two = mm(pick, grid_q[pl.ds(first * row_size, depth // CP)].reshape(depth, steps * tokens))
        rhs = [
            jnp.concatenate([jnp.where((row < HD) == (i == 0), q_two, 0.0).astype(BF16), unit], axis=0)
            for i in range(2)
        ]
        rhs.append(jnp.concatenate([r[:, tokens:] for r in rhs], axis=1))
        for k in range(3):
            rhs_v[p % 2, k] = rhs[k]

    def scores(p):
        for k, (t, _) in enumerate(jobs):
            lhs = jnp.concatenate([keys[pl.ds(t * frame_rows, frame_rows), pl.ds(p * 2 * HD, 2 * HD)], mask[t]], axis=1)
            score = mm(lhs, rhs_v[p % 2, k])
            score_v[p % 2, k] = score
            tops[p, k] = jnp.max(score, axis=0, keepdims=True)

    def weights(p):
        for k in range(3):
            weight_v[p % 2, k] = jnp.exp(score_v[p % 2, k] - tops[p, k]).astype(BF16)

    def store_part(s, h, context, total, peak):
        part[s, h, pl.ds(0, HD), :] = context
        part[s, h, pl.ds(HD, 8), :] = jnp.where(iota((8, tokens), 0) == 0, total, peak)

    def sums(p):
        result = []
        for k, (t, i) in enumerate(jobs):
            at = pl.ds(p * 2 * HD + (i or 0) * HD, 2 * HD if i is None else HD)
            lhs = jnp.concatenate([vals[at, pl.ds(t * frame_rows, frame_rows)], ones_rows], axis=0)
            result.append(mm(lhs, weight_v[p % 2, k]))
        late = result[2]
        for i in range(2):
            h = 2 * p + i
            old, top_old = result[i], tops[p, i]
            lanes = slice(i * tokens, (i + 1) * tokens)
            store_part(0, h, old[:HD, :tokens], old[HD : HD + 8, :tokens], top_old[:, :tokens] - slope[h] * dist[0])
            peak_a = top_old[:, tokens:] - slope[h] * (dist[1] + 1.0)
            peak_b = tops[p, 2][:, lanes] - slope[h] * dist[1]
            peak = jnp.maximum(peak_a, peak_b)
            fa, fb = jnp.exp(peak_a - peak), jnp.exp(peak_b - peak)
            store_part(
                1,
                h,
                fa * old[:HD, tokens:] + fb * late[i * HD : (i + 1) * HD, lanes],
                fa * old[HD : HD + 8, tokens:] + fb * late[2 * HD : 2 * HD + 8, lanes],
                peak,
            )

    def core_copy(i):
        some = pl.ds(i * nx, nx)
        return remote(part.at[other, some], pair_in.at[some], pc_s, pc_r.at[i], {"c": other})

    def x_copy(i, e):
        xx = lax.rem(x + e, nx)
        return remote(xs.at[i * nx + xx], xr.at[i, x], x_s, x_r.at[i], {"x": xx})

    def merge_group(i):
        wait_all(pair_in.at[pl.ds(0, nx)], recv=pc_r.at[i])
        for h in range(i * nx, (i + 1) * nx):
            own_part, their_part = part[c, h], pair_in[h]
            peak_a, peak_b = own_part[HD + 1 : HD + 2], their_part[HD + 1 : HD + 2]
            peak = jnp.maximum(peak_a, peak_b)
            fa, fb = jnp.exp(peak_a - peak), jnp.exp(peak_b - peak)
            merged = fa * own_part[:HD] + fb * their_part[:HD]
            total = fa * own_part[HD : HD + 1] + fb * their_part[HD : HD + 1]
            xs[h] = jnp.concatenate([merged, stats_tile(peak, total, 16)], axis=0).astype(BF16)
        for e in range(1, nx):
            x_copy(i, e).start()

    blocks, notes = {}, {}

    def gather_group(i):
        got = [xs[i * nx + x].astype(F32)]
        wait_all(xr.at[i, pl.ds(0, nx - 1)], recv=x_r.at[i])
        for e in range(1, nx):
            got.append(xr[i, lax.rem(x + e, nx)].astype(F32))
        peaks = [g[HD : HD + 1] + g[HD + 1 : HD + 2] + g[HD + 2 : HD + 3] for g in got]
        peak = functools.reduce(jnp.maximum, peaks)
        factors = [jnp.exp(one - peak) for one in peaks]
        blocks[i] = sum(f * g[:HD] for f, g in zip(factors, got))
        total = sum(f * (g[HD + 3 : HD + 4] + g[HD + 4 : HD + 5]) for f, g in zip(factors, got))
        notes[i] = stats_tile(peak, total, 8)

    gathered = 0
    for it in range(pairs + 3):
        if it < pairs:
            prepare(it)
        if 0 <= it - 1 < pairs:
            scores(it - 1)
        if 0 <= it - 2 < pairs:
            weights(it - 2)
        if 0 <= it - 3 < pairs:
            sums(it - 3)
            done, left = divmod(it - 2, per_group)
            if left == 0:
                core_copy(done - 1).start()
                if done > 1:
                    merge_group(done - 2)
    merge_group(hpx - 1)

    def z_copy(k, d):
        zz = along(d)
        return remote(zs[k].at[zz], zr[k].at[z], z_s.at[k], z_r.at[k], {"z": zz})

    def z_send(k):
        stage, span = stages[k], stage_span(stages[k])
        filled = [blocks[i] for i in stage] + [notes[i] for i in stage]
        spare = span - len(stage) * (HD + 8)
        if spare:
            filled.append(jnp.zeros((spare, tokens), F32))
        by_token = jnp.concatenate(filled, axis=0).T
        zs[k][...] = by_token.reshape(nz, per_z, span).astype(BF16)
        for d in far:
            z_copy(k, d).start()
        zr[k][z] = zs[k][z]

    def g_copy(k, d):
        return remote(ctx[k].at[z], ctx[k].at[z], g_s.at[k], g_r.at[k], {"z": along(d)})

    def z_merge(k):
        span, slots = stage_span(stages[k]), len(stages[k]) * HD
        wait_all(zr[k].at[pl.ds(0, nz - 1)], recv=z_r.at[k])
        wide = zr[k][...].astype(F32)
        flat = wide.reshape(tokens, span).astype(BF16)
        to_lane = iota((1, span), 1)
        offset = iota((span, span), 0) - slots - 8 * (to_lane >> log2(HD))
        kept = to_lane < slots
        peak_of = jnp.where(kept & (offset >= 0) & (offset < 3), 1.0, 0.0).astype(BF16)
        total_of = jnp.where(kept & (offset >= 3) & (offset < 5), 1.0, 0.0).astype(BF16)
        peaks = mm(flat, peak_of).reshape(nz, per_z, span)
        totals = mm(flat, total_of).reshape(nz, per_z, span)
        factors = jnp.exp(peaks - jnp.max(peaks, axis=0, keepdims=True))
        context = jnp.sum(factors * wide, axis=0) / jnp.sum(factors * totals, axis=0)
        context = jnp.where(iota((per_z, span), 1) < slots, context, 0.0)
        ctx[k][z] = context.astype(BF16)
        for d in far:
            g_copy(k, d).start()

    for k, stage in enumerate(stages):
        while gathered <= stage[-1]:
            gather_group(gathered)
            gathered += 1
        z_send(k)

    wait_all(wo_rows.at[pl.ds(0, row_size - 1)], recv=wo_r)
    weights_in = wo_rows[...].reshape(row_size * CP, width)
    for k, stage in enumerate(stages):
        span, slots = stage_span(stage), len(stage) * HD
        lane = iota((1, span), 1)
        source = ((stage[0] + (lane >> log2(HD))) * nx + x) * HD + (lane & (HD - 1))
        source = jnp.where(lane < slots, source, -1)
        take = jnp.where(iota((width, span), 0) == source, 1.0, 0.0).astype(BF16)
        wo_all[k][...] = mm(weights_in, take).astype(BF16)

    for k in range(ns):
        z_merge(k)

    shares = jnp.zeros((row_size * CP, tokens), F32)
    for k in range(ns):
        wait_all(ctx[k].at[pl.ds(0, nz - 1)], recv=g_r.at[k])
        rows = ctx[k][...].astype(F32).reshape(tokens, stage_span(stages[k])).astype(BF16)
        shares += mm_t(wo_all[k][...], rows)
    fin_out[...] = shares.reshape(row_size, CP, tokens)

    def f_copy(r):
        t, peer = row_peer(r)
        return remote(fin_out.at[t], fin_in.at[mine], f_s, f_r, peer)

    for r in range(1, row_size):
        f_copy(r).start()
    fin_in[mine] = fin_out[mine]

    wait_all(grid_q.at[pl.ds(0, len(first_stage + second_stage))], send=qz_s)
    wait_all(grid_q.at[pl.ds(0, nz * (nx - 1))], send=qx_s)
    wait_all(grid_q.at[pl.ds(0, nz * nx)], send=qc_s)
    wait_all(wo_rows.at[pl.ds(0, row_size - 1)], send=wo_s)
    wait_all(pair_in, send=pc_s)
    wait_all(xs.at[pl.ds(0, hpx * (nx - 1))], send=x_s)
    for k in range(ns):
        wait_all(zs[k].at[pl.ds(0, nz - 1)], send=z_s.at[k])
        wait_all(ctx[k].at[pl.ds(0, nz - 1)], send=g_s.at[k])
    wait_all(fin_in.at[pl.ds(0, row_size - 1)], recv=f_r)
    both = [sum(fin_in[xx * nc + s] for xx in range(nx))[:chunk] for s in range(steps)]
    out[...] = jnp.stack(both, axis=1).astype(BF16)
    wait_all(fin_out.at[pl.ds(0, row_size - 1)], send=f_s)


def local(frames, dec_states, w_query, w_keyval, w_output, head_slope, lengths, positions):
    nz, nx, nc = (lax.axis_size(a) for a in SEQ)
    steps, frame_rows, width = frames.shape
    tokens = dec_states.shape[1]
    heads = head_slope.shape[0]
    chunk = w_query.shape[1]
    n = nz * nx * nc
    hpx = heads // nx
    spans = [stage_span(stage) for stage in z_stages(hpx)]
    per_z = tokens // nz
    tall = steps * frame_rows
    row_size = nx * nc
    sizes = (nz, nx, nc, steps, frame_rows, tokens, width, heads, chunk)
    vmem = pl.BlockSpec(memory_space=pltpu.VMEM)
    smem = pl.BlockSpec(memory_space=pltpu.SMEM)
    dma = pltpu.SemaphoreType.DMA
    flops = 2 * tall * width * 2 * width
    out = pl.pallas_call(
        functools.partial(kernel, sizes),
        out_shape=jax.ShapeDtypeStruct((chunk, steps, tokens), BF16),
        in_specs=[pl.BlockSpec(memory_space=pl.ANY)] * 5 + [vmem] + [smem] * 2,
        out_specs=vmem,
        scratch_shapes=[
            pltpu.VMEM((tall, width), BF16),
            pltpu.VMEM((width, 2 * width), BF16),
            pltpu.VMEM((steps * tokens, width), BF16),
            pltpu.VMEM((chunk, width), BF16),
            pltpu.VMEM((chunk, width), BF16),
            pltpu.VMEM((tall, width), BF16),
            pltpu.VMEM((width, tall), BF16),
            pltpu.VMEM((steps, frame_rows, 128), BF16),
            pltpu.VMEM((n, CP, steps * tokens), BF16),
            pltpu.VMEM((CP, steps * tokens), F32),
            pltpu.VMEM((2, 3, 4 * HD, steps * tokens), BF16),
            pltpu.VMEM((2, 3, frame_rows, steps * tokens), F32),
            pltpu.VMEM((2, 3, frame_rows, steps * tokens), BF16),
            pltpu.VMEM((steps, heads, HD + 8, tokens), F32),
            pltpu.VMEM((heads, HD + 8, tokens), F32),
            pltpu.VMEM((heads, HD + 16, tokens), BF16),
            pltpu.VMEM((hpx, nx, HD + 16, tokens), BF16),
            pltpu.VMEM((row_size, CP, width), BF16),
            pltpu.VMEM((row_size, CP, tokens), F32),
            pltpu.VMEM((row_size, CP, tokens), F32),
            *[pltpu.VMEM((nz, per_z, span), BF16) for _ in range(3) for span in spans],
            *[pltpu.VMEM((row_size * CP, span), BF16) for span in spans],
            dma((steps,)),
            dma((2 * width // COLS,)),
            dma((3,)),
            dma,
            dma((nz,)),
            dma,
            dma((nz,)),
            dma,
            dma((nz,)),
            dma,
            dma,
            dma,
            dma((hpx,)),
            dma,
            dma((hpx,)),
            dma((len(spans),)),
            dma((len(spans),)),
            dma((len(spans),)),
            dma((len(spans),)),
            dma,
            dma,
        ],
        compiler_params=pltpu.CompilerParams(
            collective_id=0, has_side_effects=True, vmem_limit_bytes=60 * 1024 * 1024
        ),
        cost_estimate=pl.CostEstimate(flops=flops, bytes_accessed=2 * width * (tall + 2 * width), transcendentals=0),
        name="attend",
    )(frames.reshape(tall, width), w_keyval, dec_states.reshape(steps * tokens, width), w_query.T, w_output.T,
      positions, lengths, head_slope)
    return out.transpose(1, 2, 0)


def solution(mesh):
    devices = mesh.devices.reshape(mesh.shape["grp"], 16, 4, 2)
    finer = Mesh(devices, ("grp",) + SEQ)
    return jax.shard_map(
        local,
        mesh=finer,
        in_specs=(
            P("grp", SEQ, None),
            P(None, "grp", None),
            P(None, SEQ),
            P(),
            P(None, SEQ),
            P(),
            P("grp", None),
            P(None, "grp"),
        ),
        out_specs=P(None, "grp", SEQ),
        check_vma=False,
    )
```

```python
import functools

import jax
import jax.numpy as jnp
from jax import lax
from jax.experimental import pallas as pl
from jax.experimental.pallas import tpu as pltpu
from jax.sharding import Mesh
from jax.sharding import PartitionSpec as P

SEQ = ("z", "x", "c")
F32, BF16 = jnp.float32, jnp.bfloat16
HD = 64
CP = 16
COLS = 256
LOW = -1e30


def mm(a, b):
    return jnp.dot(a, b, preferred_element_type=F32)


def mm_t(a, b):
    return lax.dot_general(a, b, (((1,), (1,)), ((), ())), preferred_element_type=F32)


def iota(shape, dim):
    return lax.broadcasted_iota(jnp.int32, shape, dim)


def remote(src, dst, send, recv, device):
    return pltpu.make_async_remote_copy(
        src_ref=src,
        dst_ref=dst,
        send_sem=send,
        recv_sem=recv,
        device_id=device,
        device_id_type=pl.DeviceIdType.MESH,
    )


def near_first(n):
    order = []
    for d in range(1, n // 2 + 1):
        order.append(d)
        if n - d != d:
            order.append(n - d)
    return order


def pieces(value, count):
    parts = []
    for _ in range(count):
        part = value.astype(BF16).astype(F32)
        parts.append(part)
        value = value - part
    return parts


def log2(k):
    assert k & (k - 1) == 0
    return k.bit_length() - 1


def window(p, chunk, row_size):
    return 2 * HD * p // chunk // row_size, (2 * HD * (p + 1) - 1) // chunk // row_size + 1


def z_stages(hpx):
    return [tuple(range(hpx))]


def stage_span(stage):
    return -(-len(stage) * (HD + 8) // 128) * 128


def stats_tile(peak, total, rows):
    at = iota((rows, peak.shape[-1]), 0)
    tile = jnp.zeros((rows, peak.shape[-1]), F32)
    for k, part in enumerate(pieces(peak, 3) + pieces(total, 2)):
        tile = jnp.where(at == k, part, tile)
    return tile


def kernel(
    sizes,
    frames, wkv, dec, wq, wo, pos, lens, slope,
    out,
    *scratch,
):
    nz, nx, nc, steps, frame_rows, tokens, width, heads, chunk = sizes
    n = nz * nx * nc
    z, x, c = lax.axis_index("z"), lax.axis_index("x"), lax.axis_index("c")
    row_size = nx * nc
    mine = x * nc + c
    own = z * row_size + mine
    other = 1 - c
    near = near_first(nz)
    far = near[::-1]
    reach = nz // 4
    hpx = heads // nx
    pairs = heads // 2
    per_group = nx // 2
    stages = z_stages(hpx)
    ns = len(stages)
    it_ = iter(scratch)
    fr, wt, dec_v, wq_v, wo_v, keys, vals, mask, grid_q, qpad, rhs_v, score_v, weight_v, part, pair_in, xs, xr, wo_rows, fin_out, fin_in = (
        next(it_) for _ in range(20)
    )
    zs, zr, ctx, wo_all = ([next(it_) for _ in stages] for _ in range(4))
    fr_sem, wt_sem, in_sem, qz_s, qz_r, qx_s, qx_r, qc_s, qc_r, wo_s, wo_r, pc_s, pc_r, x_s, x_r, z_s, z_r, g_s, g_r, f_s, f_r = it_
    per_z = tokens // nz
    tall = steps * frame_rows
    tiles = 2 * width // COLS
    mesh_id = pl.DeviceIdType.MESH

    def along(d):
        return lax.rem(z + d + nz, nz)

    def slot(zz, xx, cc):
        return (zz * nc + cc) * nx + xx

    def wait_all(ref, send=None, recv=None):
        if send is not None:
            remote(ref, ref, send, send, {"c": 1 - c}).wait_send()
        else:
            remote(ref, ref, recv, recv, {"c": 1 - c}).wait_recv()

    def row_peer(r):
        t = lax.rem(mine + r, row_size)
        return t, {"x": t // nc, "c": lax.rem(t, nc)}

    small = [
        pltpu.make_async_copy(src, dst, in_sem.at[k]) for k, (src, dst) in enumerate(((dec, dec_v), (wq, wq_v), (wo, wo_v)))
    ]
    loads = [
        pltpu.make_async_copy(frames.at[pl.ds(k * frame_rows, frame_rows), :], fr.at[pl.ds(k * frame_rows, frame_rows), :], fr_sem.at[k])
        for k in range(steps)
    ]

    def tile_load(j):
        cols = pl.ds(pl.multiple_of(j * COLS, COLS), COLS)
        return pltpu.make_async_copy(wkv.at[:, cols], wt.at[:, cols], wt_sem.at[j])

    for load in small + loads:
        load.start()
    tile_load(0).start()

    barrier = pltpu.get_barrier_semaphore()
    close = [k for d in range(1, reach + 1) for k in (d, -d)]
    for d in close[::-1]:
        pl.semaphore_signal(barrier, inc=1, device_id={"z": along(d)}, device_id_type=mesh_id)
    for r in range(1, row_size):
        pl.semaphore_signal(barrier, inc=1, device_id=row_peer(r)[1], device_id_type=mesh_id)

    qpad[...] = jnp.zeros_like(qpad)
    small[0].wait()
    small[1].wait()
    qpad[:chunk] = mm_t(wq_v[...], dec_v[...])
    grid_q[slot(z, x, c)] = qpad[...].astype(BF16)
    pl.semaphore_wait(barrier, len(close) + row_size - 1)

    def q_chunk(zz, xx, cc):
        return grid_q.at[slot(zz, xx, cc)]

    def q_over_z(source, d):
        here = q_chunk(source, x, c)
        return remote(here, here, qz_s, qz_r.at[source], {"z": along(d)})

    def q_over_x(zz, d):
        here = q_chunk(zz, x, c)
        return remote(here, here, qx_s, qx_r.at[zz], {"x": lax.rem(x + d, nx)})

    def q_over_c(zz, cc):
        here = grid_q.at[pl.ds(slot(zz, 0, cc), nx)]
        return remote(here, here, qc_s, qc_r.at[zz], {"c": other})

    first_stage = [(z, d) for d in close[::-1]]
    second_stage = [(along(-reach), d) for d in range(reach, 0, -1)]
    second_stage += [(along(reach), -d) for d in range(reach - 1, 0, -1)]
    for args in first_stage:
        q_over_z(*args).start()

    def wo_over_row(r):
        return remote(wo_rows.at[mine], wo_rows.at[mine], wo_s, wo_r, row_peer(r)[1])

    def spread(zz):
        for e in range(1, nx):
            q_over_x(zz, e).start()

    def arrive_z(zz):
        here = q_chunk(zz, x, c)
        wait_all(here, recv=qz_r.at[zz])

    def relay():
        arrive_z(along(-reach))
        arrive_z(along(reach))
        for args in second_stage:
            q_over_z(*args).start()
        for d in (-reach, reach):
            spread(along(d))

    def spread_near():
        for d in close:
            if abs(d) < reach:
                arrive_z(along(d))
                spread(along(d))

    distant = [*range(reach + 1, nz // 2), *range(-nz // 2 + 1, -reach), nz // 2]

    def spread_far():
        for d in distant:
            arrive_z(along(d))
            spread(along(d))

    crossed = [0, 0]

    def cross_rows(after):
        for zz in range(crossed[0], after):
            wait_all(grid_q.at[pl.ds(0, nx - 1)], recv=qx_r.at[zz])
            q_over_c(zz, c).start()
        crossed[0] = max(crossed[0], after)

    spread(z)
    small[2].wait()
    wo_rows[mine] = jnp.zeros((CP, width), BF16)
    wo_rows[mine, :chunk, :] = wo_v[...]
    for r in range(1, row_size):
        wo_over_row(r).start()

    at_lane = iota((frame_rows, 128), 1)
    at_row = iota((frame_rows, 128), 0)
    for t in range(steps):
        hidden = (at_lane == 0) & (at_row >= lens[t, own])
        mask[t] = jnp.where(hidden, LOW, 0.0).astype(BF16)
    loads[0].wait()
    tile_load(0).wait()
    for j in range(1, tiles):
        tile_load(j).start()

    for t in range(steps):
        if t:
            loads[t].wait()
        rows = pl.ds(t * frame_rows, frame_rows)
        keys[rows, :COLS] = mm(fr[rows, :], wt[:, :COLS]).astype(BF16)
    half = tiles // 2

    def project_keys(j, carry):
        tile_load(j).wait()
        cols = pl.ds(pl.multiple_of(j * COLS, COLS), COLS)
        keys[:, cols] = mm(fr[...], wt[:, cols]).astype(BF16)

        @pl.when(j == max(half // 2, 1))
        def _():
            relay()

        @pl.when(j == max(half - 2, 1))
        def _():
            spread_near()

        return carry

    def project_values(j, carry):
        tile_load(j + half).wait()
        cols = pl.ds(pl.multiple_of(j * COLS + width, COLS), COLS)
        head_rows = pl.ds(pl.multiple_of(j * COLS, COLS), COLS)
        vals[head_rows, :] = mm(fr[...], wt[:, cols]).astype(BF16).T

        @pl.when(j == min(half // 2 - 1, half - 2))
        def _():
            spread_far()

        @pl.when(j == half - 2)
        def _():
            cross_rows(window(min(1, pairs - 1), chunk, row_size)[1])

        return carry

    lax.fori_loop(1, half, project_keys, 0)
    lax.fori_loop(0, half, project_values, 0)

    place = lax.rem(own + 1, n).astype(F32)
    dist = [jnp.abs(pos[pl.ds(s, 1), :].astype(F32) - place) / n for s in range(steps)]
    ones_rows = jnp.ones((16, frame_rows), BF16)
    row = iota((2 * HD, steps * tokens), 0)
    unit = jnp.where(row == 0, 1.0, 0.0).astype(BF16)
    jobs = ((0, 0), (0, 1), (1, None))
    tops = {}
    def rows_for(p):
        return window(min(p, pairs - 1), chunk, row_size)[1]

    def await_rows(last, ahead):
        cross_rows(rows_for(ahead))
        for zz in range(crossed[1], rows_for(last)):
            wait_all(grid_q.at[pl.ds(0, nx)], recv=qc_r.at[zz])
        crossed[1] = max(crossed[1], rows_for(last))

    def prepare(p):
        first, after = window(p, chunk, row_size)
        depth = (after - first) * row_size * CP
        at = iota((1, depth), 1)
        inner = at & (CP - 1)
        number = at >> log2(CP)
        in_row = ((number & (nx - 1)) << log2(nc)) + ((number >> log2(nx)) & (nc - 1))
        device = first * row_size + (number & -row_size) + in_row
        dim = jnp.where(inner < chunk, chunk * device + inner - 2 * HD * p, -1)
        pick = jnp.where(iota((2 * HD, depth), 0) == dim, HD**-0.5, 0.0).astype(BF16)
        q_two = mm(pick, grid_q[pl.ds(first * row_size, depth // CP)].reshape(depth, steps * tokens))
        rhs = [
            jnp.concatenate([jnp.where((row < HD) == (i == 0), q_two, 0.0).astype(BF16), unit], axis=0)
            for i in range(2)
        ]
        rhs.append(jnp.concatenate([r[:, tokens:] for r in rhs], axis=1))
        for k in range(3):
            rhs_v[p % 2, k] = rhs[k]

    def scores(p):
        for k, (t, _) in enumerate(jobs):
            lhs = jnp.concatenate([keys[pl.ds(t * frame_rows, frame_rows), pl.ds(p * 2 * HD, 2 * HD)], mask[t]], axis=1)
            score = mm(lhs, rhs_v[p % 2, k])
            score_v[p % 2, k] = score
            tops[p, k] = jnp.max(score, axis=0, keepdims=True)

    def weights(p):
        for k in range(3):
            weight_v[p % 2, k] = jnp.exp(score_v[p % 2, k] - tops[p, k]).astype(BF16)

    def store_part(s, h, context, total, peak):
        part[s, h, pl.ds(0, HD), :] = context
        part[s, h, pl.ds(HD, 8), :] = jnp.where(iota((8, tokens), 0) == 0, total, peak)

    def sums(p):
        result = []
        for k, (t, i) in enumerate(jobs):
            at = pl.ds(p * 2 * HD + (i or 0) * HD, 2 * HD if i is None else HD)
            lhs = jnp.concatenate([vals[at, pl.ds(t * frame_rows, frame_rows)], ones_rows], axis=0)
            result.append(mm(lhs, weight_v[p % 2, k]))
        late = result[2]
        for i in range(2):
            h = 2 * p + i
            old, top_old = result[i], tops[p, i]
            lanes = slice(i * tokens, (i + 1) * tokens)
            store_part(0, h, old[:HD, :tokens], old[HD : HD + 8, :tokens], top_old[:, :tokens] - slope[h] * dist[0])
            peak_a = top_old[:, tokens:] - slope[h] * (dist[1] + 1.0)
            peak_b = tops[p, 2][:, lanes] - slope[h] * dist[1]
            peak = jnp.maximum(peak_a, peak_b)
            fa, fb = jnp.exp(peak_a - peak), jnp.exp(peak_b - peak)
            store_part(
                1,
                h,
                fa * old[:HD, tokens:] + fb * late[i * HD : (i + 1) * HD, lanes],
                fa * old[HD : HD + 8, tokens:] + fb * late[2 * HD : 2 * HD + 8, lanes],
                peak,
            )

    def core_copy(i):
        some = pl.ds(i * nx, nx)
        return remote(part.at[other, some], pair_in.at[some], pc_s, pc_r.at[i], {"c": other})

    def x_copy(i, e):
        xx = lax.rem(x + e, nx)
        return remote(xs.at[i * nx + xx], xr.at[i, x], x_s, x_r.at[i], {"x": xx})

    def merge_group(i):
        wait_all(pair_in.at[pl.ds(0, nx)], recv=pc_r.at[i])
        for h in range(i * nx, (i + 1) * nx):
            own_part, their_part = part[c, h], pair_in[h]
            peak_a, peak_b = own_part[HD + 1 : HD + 2], their_part[HD + 1 : HD + 2]
            peak = jnp.maximum(peak_a, peak_b)
            fa, fb = jnp.exp(peak_a - peak), jnp.exp(peak_b - peak)
            merged = fa * own_part[:HD] + fb * their_part[:HD]
            total = fa * own_part[HD : HD + 1] + fb * their_part[HD : HD + 1]
            xs[h] = jnp.concatenate([merged, stats_tile(peak, total, 16)], axis=0).astype(BF16)
        for e in range(1, nx):
            x_copy(i, e).start()

    blocks, notes = {}, {}

    def gather_group(i):
        got = [xs[i * nx + x].astype(F32)]
        wait_all(xr.at[i, pl.ds(0, nx - 1)], recv=x_r.at[i])
        for e in range(1, nx):
            got.append(xr[i, lax.rem(x + e, nx)].astype(F32))
        peaks = [g[HD : HD + 1] + g[HD + 1 : HD + 2] + g[HD + 2 : HD + 3] for g in got]
        peak = functools.reduce(jnp.maximum, peaks)
        factors = [jnp.exp(one - peak) for one in peaks]
        blocks[i] = sum(f * g[:HD] for f, g in zip(factors, got))
        total = sum(f * (g[HD + 3 : HD + 4] + g[HD + 4 : HD + 5]) for f, g in zip(factors, got))
        notes[i] = stats_tile(peak, total, 8)

    gathered = 0
    for it in range(pairs + 3):
        done, left = divmod(it - 3, per_group)
        if left == 0 and done > 0:
            core_copy(done - 1).start()
            if done > 1:
                merge_group(done - 2)
        if it == 0:
            await_rows(0, 2)
        elif it < pairs and (it == 1 or left == 0):
            await_rows(it + per_group - 1, it + 2 * per_group - 1)
        if it < pairs:
            prepare(it)
        if 0 <= it - 1 < pairs:
            scores(it - 1)
        if 0 <= it - 2 < pairs:
            weights(it - 2)
        if 0 <= it - 3 < pairs:
            sums(it - 3)
    core_copy(hpx - 1).start()
    merge_group(hpx - 2)
    merge_group(hpx - 1)

    def z_copy(k, d):
        zz = along(d)
        return remote(zs[k].at[zz], zr[k].at[z], z_s.at[k], z_r.at[k], {"z": zz})

    def z_send(k):
        stage, span = stages[k], stage_span(stages[k])
        filled = [blocks[i] for i in stage] + [notes[i] for i in stage]
        spare = span - len(stage) * (HD + 8)
        if spare:
            filled.append(jnp.zeros((spare, tokens), F32))
        by_token = jnp.concatenate(filled, axis=0).T
        zs[k][...] = by_token.reshape(nz, per_z, span).astype(BF16)
        for d in far:
            z_copy(k, d).start()
        zr[k][z] = zs[k][z]

    def g_copy(k, d):
        return remote(ctx[k].at[z], ctx[k].at[z], g_s.at[k], g_r.at[k], {"z": along(d)})

    def z_merge(k):
        span, slots = stage_span(stages[k]), len(stages[k]) * HD
        wait_all(zr[k].at[pl.ds(0, nz - 1)], recv=z_r.at[k])
        wide = zr[k][...].astype(F32)
        flat = wide.reshape(tokens, span).astype(BF16)
        to_lane = iota((1, span), 1)
        offset = iota((span, span), 0) - slots - 8 * (to_lane >> log2(HD))
        kept = to_lane < slots
        peak_of = jnp.where(kept & (offset >= 0) & (offset < 3), 1.0, 0.0).astype(BF16)
        total_of = jnp.where(kept & (offset >= 3) & (offset < 5), 1.0, 0.0).astype(BF16)
        peaks = mm(flat, peak_of).reshape(nz, per_z, span)
        totals = mm(flat, total_of).reshape(nz, per_z, span)
        factors = jnp.exp(peaks - jnp.max(peaks, axis=0, keepdims=True))
        context = jnp.sum(factors * wide, axis=0) / jnp.sum(factors * totals, axis=0)
        context = jnp.where(iota((per_z, span), 1) < slots, context, 0.0)
        ctx[k][z] = context.astype(BF16)
        for d in far:
            g_copy(k, d).start()

    for k, stage in enumerate(stages):
        while gathered <= stage[-1]:
            gather_group(gathered)
            gathered += 1
        z_send(k)

    wait_all(wo_rows.at[pl.ds(0, row_size - 1)], recv=wo_r)
    weights_in = wo_rows[...].reshape(row_size * CP, width)
    for k, stage in enumerate(stages):
        span, slots = stage_span(stage), len(stage) * HD
        lane = iota((1, span), 1)
        source = ((stage[0] + (lane >> log2(HD))) * nx + x) * HD + (lane & (HD - 1))
        source = jnp.where(lane < slots, source, -1)
        take = jnp.where(iota((width, span), 0) == source, 1.0, 0.0).astype(BF16)
        wo_all[k][...] = mm(weights_in, take).astype(BF16)

    for k in range(ns):
        z_merge(k)

    shares = jnp.zeros((row_size * CP, tokens), F32)
    for k in range(ns):
        wait_all(ctx[k].at[pl.ds(0, nz - 1)], recv=g_r.at[k])
        rows = ctx[k][...].astype(F32).reshape(tokens, stage_span(stages[k])).astype(BF16)
        shares += mm_t(wo_all[k][...], rows)
    fin_out[...] = shares.reshape(row_size, CP, tokens)

    def f_copy(r):
        t, peer = row_peer(r)
        return remote(fin_out.at[t], fin_in.at[mine], f_s, f_r, peer)

    for r in range(1, row_size):
        f_copy(r).start()
    fin_in[mine] = fin_out[mine]

    wait_all(grid_q.at[pl.ds(0, len(first_stage + second_stage))], send=qz_s)
    wait_all(grid_q.at[pl.ds(0, nz * (nx - 1))], send=qx_s)
    wait_all(grid_q.at[pl.ds(0, nz * nx)], send=qc_s)
    wait_all(wo_rows.at[pl.ds(0, row_size - 1)], send=wo_s)
    wait_all(pair_in, send=pc_s)
    wait_all(xs.at[pl.ds(0, hpx * (nx - 1))], send=x_s)
    for k in range(ns):
        wait_all(zs[k].at[pl.ds(0, nz - 1)], send=z_s.at[k])
        wait_all(ctx[k].at[pl.ds(0, nz - 1)], send=g_s.at[k])
    wait_all(fin_in.at[pl.ds(0, row_size - 1)], recv=f_r)
    both = [sum(fin_in[xx * nc + s] for xx in range(nx))[:chunk] for s in range(steps)]
    out[...] = jnp.stack(both, axis=1).astype(BF16)
    wait_all(fin_out.at[pl.ds(0, row_size - 1)], send=f_s)


def local(frames, dec_states, w_query, w_keyval, w_output, head_slope, lengths, positions):
    nz, nx, nc = (lax.axis_size(a) for a in SEQ)
    steps, frame_rows, width = frames.shape
    tokens = dec_states.shape[1]
    heads = head_slope.shape[0]
    chunk = w_query.shape[1]
    n = nz * nx * nc
    hpx = heads // nx
    spans = [stage_span(stage) for stage in z_stages(hpx)]
    per_z = tokens // nz
    tall = steps * frame_rows
    row_size = nx * nc
    sizes = (nz, nx, nc, steps, frame_rows, tokens, width, heads, chunk)
    vmem = pl.BlockSpec(memory_space=pltpu.VMEM)
    smem = pl.BlockSpec(memory_space=pltpu.SMEM)
    dma = pltpu.SemaphoreType.DMA
    flops = 2 * tall * width * 2 * width
    out = pl.pallas_call(
        functools.partial(kernel, sizes),
        out_shape=jax.ShapeDtypeStruct((chunk, steps, tokens), BF16),
        in_specs=[pl.BlockSpec(memory_space=pl.ANY)] * 5 + [vmem] + [smem] * 2,
        out_specs=vmem,
        scratch_shapes=[
            pltpu.VMEM((tall, width), BF16),
            pltpu.VMEM((width, 2 * width), BF16),
            pltpu.VMEM((steps * tokens, width), BF16),
            pltpu.VMEM((chunk, width), BF16),
            pltpu.VMEM((chunk, width), BF16),
            pltpu.VMEM((tall, width), BF16),
            pltpu.VMEM((width, tall), BF16),
            pltpu.VMEM((steps, frame_rows, 128), BF16),
            pltpu.VMEM((n, CP, steps * tokens), BF16),
            pltpu.VMEM((CP, steps * tokens), F32),
            pltpu.VMEM((2, 3, 4 * HD, steps * tokens), BF16),
            pltpu.VMEM((2, 3, frame_rows, steps * tokens), F32),
            pltpu.VMEM((2, 3, frame_rows, steps * tokens), BF16),
            pltpu.VMEM((steps, heads, HD + 8, tokens), F32),
            pltpu.VMEM((heads, HD + 8, tokens), F32),
            pltpu.VMEM((heads, HD + 16, tokens), BF16),
            pltpu.VMEM((hpx, nx, HD + 16, tokens), BF16),
            pltpu.VMEM((row_size, CP, width), BF16),
            pltpu.VMEM((row_size, CP, tokens), F32),
            pltpu.VMEM((row_size, CP, tokens), F32),
            *[pltpu.VMEM((nz, per_z, span), BF16) for _ in range(3) for span in spans],
            *[pltpu.VMEM((row_size * CP, span), BF16) for span in spans],
            dma((steps,)),
            dma((2 * width // COLS,)),
            dma((3,)),
            dma,
            dma((nz,)),
            dma,
            dma((nz,)),
            dma,
            dma((nz,)),
            dma,
            dma,
            dma,
            dma((hpx,)),
            dma,
            dma((hpx,)),
            dma((len(spans),)),
            dma((len(spans),)),
            dma((len(spans),)),
            dma((len(spans),)),
            dma,
            dma,
        ],
        compiler_params=pltpu.CompilerParams(
            collective_id=0, has_side_effects=True, vmem_limit_bytes=60 * 1024 * 1024
        ),
        cost_estimate=pl.CostEstimate(flops=flops, bytes_accessed=2 * width * (tall + 2 * width), transcendentals=0),
        name="attend",
    )(frames.reshape(tall, width), w_keyval, dec_states.reshape(steps * tokens, width), w_query.T, w_output.T,
      positions, lengths, head_slope)
    return out.transpose(1, 2, 0)


def solution(mesh):
    devices = mesh.devices.reshape(mesh.shape["grp"], 16, 4, 2)
    finer = Mesh(devices, ("grp",) + SEQ)
    return jax.shard_map(
        local,
        mesh=finer,
        in_specs=(
            P("grp", SEQ, None),
            P(None, "grp", None),
            P(None, SEQ),
            P(),
            P(None, SEQ),
            P(),
            P("grp", None),
            P(None, "grp"),
        ),
        out_specs=P(None, "grp", SEQ),
        check_vma=False,
    )
```

```python
import functools

import jax
import jax.numpy as jnp
from jax import lax
from jax.experimental import pallas as pl
from jax.experimental.pallas import tpu as pltpu
from jax.sharding import Mesh
from jax.sharding import PartitionSpec as P

SEQ = ("z", "x", "c")
F32, BF16 = jnp.float32, jnp.bfloat16
HD = 64
CP = 16
COLS = 256
LOW = -1e30


def mm(a, b):
    return jnp.dot(a, b, preferred_element_type=F32)


def mm_t(a, b):
    return lax.dot_general(a, b, (((1,), (1,)), ((), ())), preferred_element_type=F32)


def iota(shape, dim):
    return lax.broadcasted_iota(jnp.int32, shape, dim)


def remote(src, dst, send, recv, device):
    return pltpu.make_async_remote_copy(
        src_ref=src,
        dst_ref=dst,
        send_sem=send,
        recv_sem=recv,
        device_id=device,
        device_id_type=pl.DeviceIdType.MESH,
    )


def near_first(n):
    order = []
    for d in range(1, n // 2 + 1):
        order.append(d)
        if n - d != d:
            order.append(n - d)
    return order


def pieces(value, count):
    parts = []
    for _ in range(count):
        part = value.astype(BF16).astype(F32)
        parts.append(part)
        value = value - part
    return parts


def log2(k):
    assert k & (k - 1) == 0
    return k.bit_length() - 1


def window(p, chunk, row_size):
    return 2 * HD * p // chunk // row_size, (2 * HD * (p + 1) - 1) // chunk // row_size + 1


def z_stages(hpx):
    return [tuple(range(hpx))]


def stage_span(stage):
    return -(-len(stage) * (HD + 8) // 128) * 128


def stats_tile(peak, total, rows):
    at = iota((rows, peak.shape[-1]), 0)
    tile = jnp.zeros((rows, peak.shape[-1]), F32)
    for k, part in enumerate(pieces(peak, 3) + pieces(total, 2)):
        tile = jnp.where(at == k, part, tile)
    return tile


def kernel(
    sizes,
    frames, wkv, dec, wq, wo, pos, lens, slope,
    out,
    *scratch,
):
    nz, nx, nc, steps, frame_rows, tokens, width, heads, chunk = sizes
    n = nz * nx * nc
    z, x, c = lax.axis_index("z"), lax.axis_index("x"), lax.axis_index("c")
    row_size = nx * nc
    mine = x * nc + c
    own = z * row_size + mine
    other = 1 - c
    near = near_first(nz)
    far = near[::-1]
    reach = nz // 4
    hpx = heads // nx
    pairs = heads // 2
    per_group = nx // 2
    stages = z_stages(hpx)
    ns = len(stages)
    it_ = iter(scratch)
    fr, wt, dec_v, wq_v, wo_v, keys, vals, mask, grid_q, qpad, rhs_v, score_v, weight_v, part, pair_in, xs, xr, wo_rows, fin_out, fin_in = (
        next(it_) for _ in range(20)
    )
    zs, zr, ctx, wo_all = ([next(it_) for _ in stages] for _ in range(4))
    fr_sem, wt_sem, in_sem, qz_s, qz_r, qx_s, qx_r, qc_s, qc_r, wo_s, wo_r, pc_s, pc_r, x_s, x_r, z_s, z_r, g_s, g_r, f_s, f_r = it_
    per_z = tokens // nz
    tall = steps * frame_rows
    tiles = 2 * width // COLS
    mesh_id = pl.DeviceIdType.MESH

    def along(d):
        return lax.rem(z + d + nz, nz)

    def slot(zz, xx, cc):
        return (zz * nc + cc) * nx + xx

    def wait_all(ref, send=None, recv=None):
        if send is not None:
            remote(ref, ref, send, send, {"c": 1 - c}).wait_send()
        else:
            remote(ref, ref, recv, recv, {"c": 1 - c}).wait_recv()

    def row_peer(r):
        t = lax.rem(mine + r, row_size)
        return t, {"x": t // nc, "c": lax.rem(t, nc)}

    small = [
        pltpu.make_async_copy(src, dst, in_sem.at[k]) for k, (src, dst) in enumerate(((dec, dec_v), (wq, wq_v), (wo, wo_v)))
    ]
    loads = [
        pltpu.make_async_copy(frames.at[pl.ds(k * frame_rows, frame_rows), :], fr.at[pl.ds(k * frame_rows, frame_rows), :], fr_sem.at[k])
        for k in range(steps)
    ]

    def tile_load(j):
        cols = pl.ds(pl.multiple_of(j * COLS, COLS), COLS)
        return pltpu.make_async_copy(wkv.at[:, cols], wt.at[:, cols], wt_sem.at[j])

    for load in small[:2]:
        load.start()

    barrier = pltpu.get_barrier_semaphore()
    close = [k for d in range(1, reach + 1) for k in (d, -d)]
    for d in close[::-1]:
        pl.semaphore_signal(barrier, inc=1, device_id={"z": along(d)}, device_id_type=mesh_id)
    for r in range(1, row_size):
        pl.semaphore_signal(barrier, inc=1, device_id=row_peer(r)[1], device_id_type=mesh_id)
    for load in loads + small[2:]:
        load.start()
    tile_load(0).start()

    qpad[...] = jnp.zeros_like(qpad)
    small[0].wait()
    small[1].wait()
    qpad[:chunk] = mm_t(wq_v[...], dec_v[...])
    grid_q[slot(z, x, c)] = qpad[...].astype(BF16)
    pl.semaphore_wait(barrier, len(close) + row_size - 1)

    def q_chunk(zz, xx, cc):
        return grid_q.at[slot(zz, xx, cc)]

    def q_over_z(source, d):
        here = q_chunk(source, x, c)
        return remote(here, here, qz_s, qz_r.at[source], {"z": along(d)})

    def q_over_x(zz, d):
        here = q_chunk(zz, x, c)
        return remote(here, here, qx_s, qx_r.at[zz], {"x": lax.rem(x + d, nx)})

    def q_over_c(zz, cc):
        here = grid_q.at[pl.ds(slot(zz, 0, cc), nx)]
        return remote(here, here, qc_s, qc_r.at[zz], {"c": other})

    first_stage = [(z, d) for d in close[::-1]]
    second_stage = [(along(-reach), d) for d in range(reach, 0, -1)]
    second_stage += [(along(reach), -d) for d in range(reach - 1, 0, -1)]
    for args in first_stage:
        q_over_z(*args).start()

    def wo_over_row(r):
        return remote(wo_rows.at[mine], wo_rows.at[mine], wo_s, wo_r, row_peer(r)[1])

    def spread(zz):
        for e in range(1, nx):
            q_over_x(zz, e).start()

    def arrive_z(zz):
        here = q_chunk(zz, x, c)
        wait_all(here, recv=qz_r.at[zz])

    def relay():
        arrive_z(along(-reach))
        arrive_z(along(reach))
        for args in second_stage:
            q_over_z(*args).start()
        for d in (-reach, reach):
            spread(along(d))

    def spread_near():
        for d in close:
            if abs(d) < reach:
                arrive_z(along(d))
                spread(along(d))

    distant = [*range(reach + 1, nz // 2), *range(-nz // 2 + 1, -reach), nz // 2]

    def spread_far():
        for d in distant:
            arrive_z(along(d))
            spread(along(d))

    crossed = [0, 0]

    def cross_rows(after):
        for zz in range(crossed[0], after):
            wait_all(grid_q.at[pl.ds(0, nx - 1)], recv=qx_r.at[zz])
            q_over_c(zz, c).start()
        crossed[0] = max(crossed[0], after)

    spread(z)
    small[2].wait()
    wo_rows[mine] = jnp.zeros((CP, width), BF16)
    wo_rows[mine, :chunk, :] = wo_v[...]
    for r in range(1, row_size):
        wo_over_row(r).start()

    at_lane = iota((frame_rows, 128), 1)
    at_row = iota((frame_rows, 128), 0)
    for t in range(steps):
        hidden = (at_lane == 0) & (at_row >= lens[t, own])
        mask[t] = jnp.where(hidden, LOW, 0.0).astype(BF16)
    loads[0].wait()
    tile_load(0).wait()
    for j in range(1, tiles):
        tile_load(j).start()

    for t in range(steps):
        if t:
            loads[t].wait()
        rows = pl.ds(t * frame_rows, frame_rows)
        keys[rows, :COLS] = mm(fr[rows, :], wt[:, :COLS]).astype(BF16)
    half = tiles // 2

    def project_keys(j, carry):
        tile_load(j).wait()
        cols = pl.ds(pl.multiple_of(j * COLS, COLS), COLS)
        keys[:, cols] = mm(fr[...], wt[:, cols]).astype(BF16)

        @pl.when(j == max(half // 2, 1))
        def _():
            relay()

        @pl.when(j == max(half - 2, 1))
        def _():
            spread_near()

        return carry

    def project_values(j, carry):
        tile_load(j + half).wait()
        cols = pl.ds(pl.multiple_of(j * COLS + width, COLS), COLS)
        head_rows = pl.ds(pl.multiple_of(j * COLS, COLS), COLS)
        vals[head_rows, :] = mm(fr[...], wt[:, cols]).astype(BF16).T

        @pl.when(j == min(half // 2 - 1, half - 2))
        def _():
            spread_far()

        @pl.when(j == half - 2)
        def _():
            cross_rows(window(min(1, pairs - 1), chunk, row_size)[1])

        return carry

    lax.fori_loop(1, half, project_keys, 0)
    lax.fori_loop(0, half, project_values, 0)

    place = lax.rem(own + 1, n).astype(F32)
    dist = [jnp.abs(pos[pl.ds(s, 1), :].astype(F32) - place) / n for s in range(steps)]
    ones_rows = jnp.ones((16, frame_rows), BF16)
    row = iota((2 * HD, steps * tokens), 0)
    unit = jnp.where(row == 0, 1.0, 0.0).astype(BF16)
    jobs = ((0, 0), (0, 1), (1, None))
    tops = {}
    def rows_for(p):
        return window(min(p, pairs - 1), chunk, row_size)[1]

    def await_rows(last, ahead):
        cross_rows(max(rows_for(ahead), rows_for(last)))
        for zz in range(crossed[1], rows_for(last)):
            wait_all(grid_q.at[pl.ds(0, nx)], recv=qc_r.at[zz])
        crossed[1] = max(crossed[1], rows_for(last))

    def prepare(p):
        first, after = window(p, chunk, row_size)
        depth = (after - first) * row_size * CP
        at = iota((1, depth), 1)
        inner = at & (CP - 1)
        number = at >> log2(CP)
        in_row = ((number & (nx - 1)) << log2(nc)) + ((number >> log2(nx)) & (nc - 1))
        device = first * row_size + (number & -row_size) + in_row
        dim = jnp.where(inner < chunk, chunk * device + inner - 2 * HD * p, -1)
        pick = jnp.where(iota((2 * HD, depth), 0) == dim, HD**-0.5, 0.0).astype(BF16)
        q_two = mm(pick, grid_q[pl.ds(first * row_size, depth // CP)].reshape(depth, steps * tokens))
        rhs = [
            jnp.concatenate([jnp.where((row < HD) == (i == 0), q_two, 0.0).astype(BF16), unit], axis=0)
            for i in range(2)
        ]
        rhs.append(jnp.concatenate([r[:, tokens:] for r in rhs], axis=1))
        for k in range(3):
            rhs_v[p % 2, k] = rhs[k]

    def scores(p):
        for k, (t, _) in enumerate(jobs):
            lhs = jnp.concatenate([keys[pl.ds(t * frame_rows, frame_rows), pl.ds(p * 2 * HD, 2 * HD)], mask[t]], axis=1)
            score = mm(lhs, rhs_v[p % 2, k])
            score_v[p % 2, k] = score
            tops[p, k] = jnp.max(score, axis=0, keepdims=True)

    def weights(p):
        for k in range(3):
            weight_v[p % 2, k] = jnp.exp(score_v[p % 2, k] - tops[p, k]).astype(BF16)

    def store_part(s, h, context, total, peak):
        part[s, h, pl.ds(0, HD), :] = context
        part[s, h, pl.ds(HD, 8), :] = jnp.where(iota((8, tokens), 0) == 0, total, peak)

    def sums(p):
        result = []
        for k, (t, i) in enumerate(jobs):
            at = pl.ds(p * 2 * HD + (i or 0) * HD, 2 * HD if i is None else HD)
            lhs = jnp.concatenate([vals[at, pl.ds(t * frame_rows, frame_rows)], ones_rows], axis=0)
            result.append(mm(lhs, weight_v[p % 2, k]))
        late = result[2]
        for i in range(2):
            h = 2 * p + i
            old, top_old = result[i], tops[p, i]
            lanes = slice(i * tokens, (i + 1) * tokens)
            store_part(0, h, old[:HD, :tokens], old[HD : HD + 8, :tokens], top_old[:, :tokens] - slope[h] * dist[0])
            peak_a = top_old[:, tokens:] - slope[h] * (dist[1] + 1.0)
            peak_b = tops[p, 2][:, lanes] - slope[h] * dist[1]
            peak = jnp.maximum(peak_a, peak_b)
            fa, fb = jnp.exp(peak_a - peak), jnp.exp(peak_b - peak)
            store_part(
                1,
                h,
                fa * old[:HD, tokens:] + fb * late[i * HD : (i + 1) * HD, lanes],
                fa * old[HD : HD + 8, tokens:] + fb * late[2 * HD : 2 * HD + 8, lanes],
                peak,
            )

    def core_copy(i):
        some = pl.ds(i * nx, nx)
        return remote(part.at[other, some], pair_in.at[some], pc_s, pc_r.at[i], {"c": other})

    def x_copy(i, e):
        xx = lax.rem(x + e, nx)
        return remote(xs.at[i * nx + xx], xr.at[i, x], x_s, x_r.at[i], {"x": xx})

    def merge_group(i):
        wait_all(pair_in.at[pl.ds(0, nx)], recv=pc_r.at[i])
        for h in range(i * nx, (i + 1) * nx):
            own_part, their_part = part[c, h], pair_in[h]
            peak_a, peak_b = own_part[HD + 1 : HD + 2], their_part[HD + 1 : HD + 2]
            peak = jnp.maximum(peak_a, peak_b)
            fa, fb = jnp.exp(peak_a - peak), jnp.exp(peak_b - peak)
            merged = fa * own_part[:HD] + fb * their_part[:HD]
            total = fa * own_part[HD : HD + 1] + fb * their_part[HD : HD + 1]
            xs[h] = jnp.concatenate([merged, stats_tile(peak, total, 16)], axis=0).astype(BF16)
        for e in range(1, nx):
            x_copy(i, e).start()

    blocks, notes = {}, {}

    def gather_group(i):
        got = [xs[i * nx + x].astype(F32)]
        wait_all(xr.at[i, pl.ds(0, nx - 1)], recv=x_r.at[i])
        for e in range(1, nx):
            got.append(xr[i, lax.rem(x + e, nx)].astype(F32))
        peaks = [g[HD : HD + 1] + g[HD + 1 : HD + 2] + g[HD + 2 : HD + 3] for g in got]
        peak = functools.reduce(jnp.maximum, peaks)
        factors = [jnp.exp(one - peak) for one in peaks]
        blocks[i] = sum(f * g[:HD] for f, g in zip(factors, got))
        total = sum(f * (g[HD + 3 : HD + 4] + g[HD + 4 : HD + 5]) for f, g in zip(factors, got))
        notes[i] = stats_tile(peak, total, 8)

    gathered = 0
    for it in range(pairs + 3):
        done, left = divmod(it - 3, per_group)
        if left == 0 and done > 0:
            core_copy(done - 1).start()
            if done > 1:
                merge_group(done - 2)
        if it < min(3, pairs):
            await_rows(it, (1, 2, 4)[it])
        elif it < pairs and left == 0:
            await_rows(it + per_group - 1, it + 2 * per_group - 1)
        if it < pairs:
            prepare(it)
        if 0 <= it - 1 < pairs:
            scores(it - 1)
        if 0 <= it - 2 < pairs:
            weights(it - 2)
        if 0 <= it - 3 < pairs:
            sums(it - 3)
    core_copy(hpx - 1).start()
    merge_group(hpx - 2)
    merge_group(hpx - 1)

    def z_copy(k, d):
        zz = along(d)
        return remote(zs[k].at[zz], zr[k].at[z], z_s.at[k], z_r.at[k], {"z": zz})

    def z_send(k):
        stage, span = stages[k], stage_span(stages[k])
        filled = [blocks[i] for i in stage] + [notes[i] for i in stage]
        spare = span - len(stage) * (HD + 8)
        if spare:
            filled.append(jnp.zeros((spare, tokens), F32))
        by_token = jnp.concatenate(filled, axis=0).T
        zs[k][...] = by_token.reshape(nz, per_z, span).astype(BF16)
        for d in far:
            z_copy(k, d).start()
        zr[k][z] = zs[k][z]

    def g_copy(k, d):
        return remote(ctx[k].at[z], ctx[k].at[z], g_s.at[k], g_r.at[k], {"z": along(d)})

    def z_merge(k):
        span, slots = stage_span(stages[k]), len(stages[k]) * HD
        wait_all(zr[k].at[pl.ds(0, nz - 1)], recv=z_r.at[k])
        wide = zr[k][...].astype(F32)
        flat = wide.reshape(tokens, span).astype(BF16)
        to_lane = iota((1, span), 1)
        offset = iota((span, span), 0) - slots - 8 * (to_lane >> log2(HD))
        kept = to_lane < slots
        peak_of = jnp.where(kept & (offset >= 0) & (offset < 3), 1.0, 0.0).astype(BF16)
        total_of = jnp.where(kept & (offset >= 3) & (offset < 5), 1.0, 0.0).astype(BF16)
        peaks = mm(flat, peak_of).reshape(nz, per_z, span)
        totals = mm(flat, total_of).reshape(nz, per_z, span)
        factors = jnp.exp(peaks - jnp.max(peaks, axis=0, keepdims=True))
        context = jnp.sum(factors * wide, axis=0) / jnp.sum(factors * totals, axis=0)
        context = jnp.where(iota((per_z, span), 1) < slots, context, 0.0)
        ctx[k][z] = context.astype(BF16)
        for d in far:
            g_copy(k, d).start()

    for k, stage in enumerate(stages):
        while gathered <= stage[-1]:
            gather_group(gathered)
            gathered += 1
        z_send(k)

    wait_all(wo_rows.at[pl.ds(0, row_size - 1)], recv=wo_r)
    weights_in = wo_rows[...].reshape(row_size * CP, width)
    for k, stage in enumerate(stages):
        span, slots = stage_span(stage), len(stage) * HD
        lane = iota((1, span), 1)
        source = ((stage[0] + (lane >> log2(HD))) * nx + x) * HD + (lane & (HD - 1))
        source = jnp.where(lane < slots, source, -1)
        take = jnp.where(iota((width, span), 0) == source, 1.0, 0.0).astype(BF16)
        wo_all[k][...] = mm(weights_in, take).astype(BF16)

    for k in range(ns):
        z_merge(k)

    shares = jnp.zeros((row_size * CP, tokens), F32)
    for k in range(ns):
        wait_all(ctx[k].at[pl.ds(0, nz - 1)], recv=g_r.at[k])
        rows = ctx[k][...].astype(F32).reshape(tokens, stage_span(stages[k])).astype(BF16)
        shares += mm_t(wo_all[k][...], rows)
    fin_out[...] = shares.reshape(row_size, CP, tokens)

    def f_copy(r):
        t, peer = row_peer(r)
        return remote(fin_out.at[t], fin_in.at[mine], f_s, f_r, peer)

    for r in range(1, row_size):
        f_copy(r).start()
    fin_in[mine] = fin_out[mine]

    wait_all(grid_q.at[pl.ds(0, len(first_stage + second_stage))], send=qz_s)
    wait_all(grid_q.at[pl.ds(0, nz * (nx - 1))], send=qx_s)
    wait_all(grid_q.at[pl.ds(0, nz * nx)], send=qc_s)
    wait_all(wo_rows.at[pl.ds(0, row_size - 1)], send=wo_s)
    wait_all(pair_in, send=pc_s)
    wait_all(xs.at[pl.ds(0, hpx * (nx - 1))], send=x_s)
    for k in range(ns):
        wait_all(zs[k].at[pl.ds(0, nz - 1)], send=z_s.at[k])
        wait_all(ctx[k].at[pl.ds(0, nz - 1)], send=g_s.at[k])
    wait_all(fin_in.at[pl.ds(0, row_size - 1)], recv=f_r)
    both = [sum(fin_in[xx * nc + s] for xx in range(nx))[:chunk] for s in range(steps)]
    out[...] = jnp.stack(both, axis=1).astype(BF16)
    wait_all(fin_out.at[pl.ds(0, row_size - 1)], send=f_s)


def local(frames, dec_states, w_query, w_keyval, w_output, head_slope, lengths, positions):
    nz, nx, nc = (lax.axis_size(a) for a in SEQ)
    steps, frame_rows, width = frames.shape
    tokens = dec_states.shape[1]
    heads = head_slope.shape[0]
    chunk = w_query.shape[1]
    n = nz * nx * nc
    hpx = heads // nx
    spans = [stage_span(stage) for stage in z_stages(hpx)]
    per_z = tokens // nz
    tall = steps * frame_rows
    row_size = nx * nc
    sizes = (nz, nx, nc, steps, frame_rows, tokens, width, heads, chunk)
    vmem = pl.BlockSpec(memory_space=pltpu.VMEM)
    smem = pl.BlockSpec(memory_space=pltpu.SMEM)
    dma = pltpu.SemaphoreType.DMA
    flops = 2 * tall * width * 2 * width
    out = pl.pallas_call(
        functools.partial(kernel, sizes),
        out_shape=jax.ShapeDtypeStruct((chunk, steps, tokens), BF16),
        in_specs=[pl.BlockSpec(memory_space=pl.ANY)] * 5 + [vmem] + [smem] * 2,
        out_specs=vmem,
        scratch_shapes=[
            pltpu.VMEM((tall, width), BF16),
            pltpu.VMEM((width, 2 * width), BF16),
            pltpu.VMEM((steps * tokens, width), BF16),
            pltpu.VMEM((chunk, width), BF16),
            pltpu.VMEM((chunk, width), BF16),
            pltpu.VMEM((tall, width), BF16),
            pltpu.VMEM((width, tall), BF16),
            pltpu.VMEM((steps, frame_rows, 128), BF16),
            pltpu.VMEM((n, CP, steps * tokens), BF16),
            pltpu.VMEM((CP, steps * tokens), F32),
            pltpu.VMEM((2, 3, 4 * HD, steps * tokens), BF16),
            pltpu.VMEM((2, 3, frame_rows, steps * tokens), F32),
            pltpu.VMEM((2, 3, frame_rows, steps * tokens), BF16),
            pltpu.VMEM((steps, heads, HD + 8, tokens), F32),
            pltpu.VMEM((heads, HD + 8, tokens), F32),
            pltpu.VMEM((heads, HD + 16, tokens), BF16),
            pltpu.VMEM((hpx, nx, HD + 16, tokens), BF16),
            pltpu.VMEM((row_size, CP, width), BF16),
            pltpu.VMEM((row_size, CP, tokens), F32),
            pltpu.VMEM((row_size, CP, tokens), F32),
            *[pltpu.VMEM((nz, per_z, span), BF16) for _ in range(3) for span in spans],
            *[pltpu.VMEM((row_size * CP, span), BF16) for span in spans],
            dma((steps,)),
            dma((2 * width // COLS,)),
            dma((3,)),
            dma,
            dma((nz,)),
            dma,
            dma((nz,)),
            dma,
            dma((nz,)),
            dma,
            dma,
            dma,
            dma((hpx,)),
            dma,
            dma((hpx,)),
            dma((len(spans),)),
            dma((len(spans),)),
            dma((len(spans),)),
            dma((len(spans),)),
            dma,
            dma,
        ],
        compiler_params=pltpu.CompilerParams(
            collective_id=0, has_side_effects=True, vmem_limit_bytes=60 * 1024 * 1024
        ),
        cost_estimate=pl.CostEstimate(flops=flops, bytes_accessed=2 * width * (tall + 2 * width), transcendentals=0),
        name="attend",
    )(frames.reshape(tall, width), w_keyval, dec_states.reshape(steps * tokens, width), w_query.T, w_output.T,
      positions, lengths, head_slope)
    return out.transpose(1, 2, 0)


def solution(mesh):
    devices = mesh.devices.reshape(mesh.shape["grp"], 16, 4, 2)
    finer = Mesh(devices, ("grp",) + SEQ)
    return jax.shard_map(
        local,
        mesh=finer,
        in_specs=(
            P("grp", SEQ, None),
            P(None, "grp", None),
            P(None, SEQ),
            P(),
            P(None, SEQ),
            P(),
            P("grp", None),
            P(None, "grp"),
        ),
        out_specs=P(None, "grp", SEQ),
        check_vma=False,
    )
```
